8 devices in a mesh: batch: 1 (over z), time: 2 (over y), region: 4 (over x, core).
Axes of the slice: x: 2, y: 2, z: 1, core: 2. Of those that a mesh axis runs over, the one named last changes fastest.
Arguments:
- patches: bfloat16 [2048, 1536], P(('batch', 'time', 'region'))
- enc_pos: bfloat16 [2048, 1280], P(('batch', 'time', 'region'))
- vis_mask: int32 [2048], P(('batch', 'time', 'region'))
- dec_pos: bfloat16 [2048, 512], P(('batch', 'time', 'region'))
- w_embed: bfloat16 [1536, 1280], replicated
- b_embed: float32 [1280], replicated
- enc_vec: float32 [2, 12, 1280], replicated
- enc_wqkv: bfloat16 [2, 1280, 3, 16, 80], replicated
- enc_wo: bfloat16 [2, 16, 80, 1280], replicated
- enc_w1: bfloat16 [2, 1280, 5120], replicated
- enc_w2: bfloat16 [2, 5120, 1280], replicated
- enc_final: float32 [2, 1280], replicated
- w_dec_in: bfloat16 [1280, 512], replicated
- mask_token: bfloat16 [512], replicated
- dec_vec: float32 [2, 12, 512], replicated
- dec_wqkv: bfloat16 [2, 512, 3, 16, 32], replicated
- dec_wo: bfloat16 [2, 16, 32, 512], replicated
- dec_w1: bfloat16 [2, 512, 2048], replicated
- dec_w2: bfloat16 [2, 2048, 512], replicated
- dec_final: float32 [2, 512], replicated
- w_out: bfloat16 [512, 1536], replicated
Outputs:
- output: float32 [2048, 1536], P(('batch', 'time', 'region'))
All inputs are finite; a program needn't handle non-finite values.
Results may differ from the reference program's by a relative error of at most 0.0172449.
Values are sent between devices in bfloat16 or wider.
A program may use at most 1 GiB of HBM per device.

```python
import jax
import jax.numpy as jnp
from jax import lax

PATCH_DIM = 1536
ENC_WIDTH = 1280
ENC_HEADS = 16
DEC_WIDTH = 512
DEC_HEADS = 16
TOKENS_DEV = 256
TIME_BLOCKS = 2
REGIONS = 4
KEEP_DIV = 8
ENC_LAYERS = 2
DEC_LAYERS = 2

SHARDS = TIME_BLOCKS * REGIONS
TOKENS = TOKENS_DEV * SHARDS
VIS_DEV = TOKENS_DEV // KEEP_DIV
VISIBLE = VIS_DEV * SHARDS
SKEW = min(4, REGIONS)
ENC_HEAD = ENC_WIDTH // ENC_HEADS
DEC_HEAD = DEC_WIDTH // DEC_HEADS
LN_EPS = 1e-6


def draw_mask(mask_key):
    key_rank, key_shift, key_place = jax.random.split(mask_key, 3)
    pair_count = (REGIONS - SKEW) // 2
    shifts = jax.random.randint(key_shift, (TIME_BLOCKS, pair_count), 0, VIS_DEV + 1)
    paired = jnp.stack([VIS_DEV + shifts, VIS_DEV - shifts], axis=-1).reshape(TIME_BLOCKS, REGIONS - SKEW)
    profile = jnp.concatenate([jnp.full((TIME_BLOCKS, 1), SKEW * VIS_DEV, jnp.int32), jnp.zeros((TIME_BLOCKS, SKEW - 1), jnp.int32), paired.astype(jnp.int32)], axis=1)
    region_rank = jax.vmap(lambda one_key: jax.random.permutation(one_key, REGIONS))(jax.random.split(key_rank, TIME_BLOCKS))
    counts = jnp.take_along_axis(profile, region_rank, axis=1).reshape(SHARDS, 1)
    token_rank = jax.vmap(lambda one_key: jax.random.permutation(one_key, TOKENS_DEV))(jax.random.split(key_place, SHARDS))
    return (token_rank < counts).astype(jnp.int32).reshape(TOKENS)


def normal_draw(draw_key, out_shape, spread):
    return jax.random.normal(draw_key, out_shape, jnp.float32) * spread


def qkv_gain():
    return jnp.array([1.6, 1.6, 1.0], jnp.float32)[:, None, None]


def block_vectors(draw_key, layer_count, model_width):
    gain_rows = jnp.array([1.0, 0.0, 1.0, 0.0, 0.0, 0.0, 0.0, 0.0, 0.0, 0.0, 0.0, 0.0], jnp.float32)[:, None]
    return jax.random.normal(draw_key, (layer_count, 12, model_width), jnp.float32) * 0.2 + gain_rows


def final_vectors(draw_key, model_width):
    return jax.random.normal(draw_key, (2, model_width), jnp.float32) * 0.2 + jnp.array([1.0, 0.0], jnp.float32)[:, None]


def setup_inputs(seed: int = 0, part: int = 0) -> dict:
    part_key = jax.random.fold_in(jax.random.key(seed), part)
    key_patch, key_epos, key_mask, key_dpos = jax.random.split(part_key, 4)
    weight_keys = jax.random.split(jax.random.key(seed + 1), 17)
    return {
        "patches": normal_draw(key_patch, (TOKENS, PATCH_DIM), 1.0).astype(jnp.bfloat16),
        "enc_pos": normal_draw(key_epos, (TOKENS, ENC_WIDTH), 0.5).astype(jnp.bfloat16),
        "vis_mask": draw_mask(key_mask),
        "dec_pos": normal_draw(key_dpos, (TOKENS, DEC_WIDTH), 0.5).astype(jnp.bfloat16),
        "w_embed": normal_draw(weight_keys[0], (PATCH_DIM, ENC_WIDTH), PATCH_DIM ** -0.5).astype(jnp.bfloat16),
        "b_embed": normal_draw(weight_keys[1], (ENC_WIDTH,), 0.5),
        "enc_vec": block_vectors(weight_keys[2], ENC_LAYERS, ENC_WIDTH),
        "enc_wqkv": (normal_draw(weight_keys[3], (ENC_LAYERS, ENC_WIDTH, 3, ENC_HEADS, ENC_HEAD), ENC_WIDTH ** -0.5) * qkv_gain()).astype(jnp.bfloat16),
        "enc_wo": normal_draw(weight_keys[4], (ENC_LAYERS, ENC_HEADS, ENC_HEAD, ENC_WIDTH), 1.5 * ENC_WIDTH ** -0.5).astype(jnp.bfloat16),
        "enc_w1": normal_draw(weight_keys[5], (ENC_LAYERS, ENC_WIDTH, 4 * ENC_WIDTH), ENC_WIDTH ** -0.5).astype(jnp.bfloat16),
        "enc_w2": normal_draw(weight_keys[6], (ENC_LAYERS, 4 * ENC_WIDTH, ENC_WIDTH), (4 * ENC_WIDTH) ** -0.5).astype(jnp.bfloat16),
        "enc_final": final_vectors(weight_keys[7], ENC_WIDTH),
        "w_dec_in": normal_draw(weight_keys[8], (ENC_WIDTH, DEC_WIDTH), 1.5 * ENC_WIDTH ** -0.5).astype(jnp.bfloat16),
        "mask_token": normal_draw(weight_keys[9], (DEC_WIDTH,), 1.0).astype(jnp.bfloat16),
        "dec_vec": block_vectors(weight_keys[10], DEC_LAYERS, DEC_WIDTH),
        "dec_wqkv": (normal_draw(weight_keys[11], (DEC_LAYERS, DEC_WIDTH, 3, DEC_HEADS, DEC_HEAD), DEC_WIDTH ** -0.5) * qkv_gain()).astype(jnp.bfloat16),
        "dec_wo": normal_draw(weight_keys[12], (DEC_LAYERS, DEC_HEADS, DEC_HEAD, DEC_WIDTH), 1.5 * DEC_WIDTH ** -0.5).astype(jnp.bfloat16),
        "dec_w1": normal_draw(weight_keys[13], (DEC_LAYERS, DEC_WIDTH, 4 * DEC_WIDTH), DEC_WIDTH ** -0.5).astype(jnp.bfloat16),
        "dec_w2": normal_draw(weight_keys[14], (DEC_LAYERS, 4 * DEC_WIDTH, DEC_WIDTH), (4 * DEC_WIDTH) ** -0.5).astype(jnp.bfloat16),
        "dec_final": final_vectors(weight_keys[15], DEC_WIDTH),
        "w_out": normal_draw(weight_keys[16], (DEC_WIDTH, PATCH_DIM), DEC_WIDTH ** -0.5).astype(jnp.bfloat16),
    }


def layer_norm(hidden, ln_gain, ln_shift):
    hid_f32 = hidden.astype(jnp.float32)
    mean_val = jnp.mean(hid_f32, axis=-1, keepdims=True)
    centered = hid_f32 - mean_val
    variance = jnp.mean(centered * centered, axis=-1, keepdims=True)
    return centered * lax.rsqrt(variance + LN_EPS) * ln_gain + ln_shift


def attention(query_rows, key_rows, value_rows, blocks):
    query_count, head_count, head_dim = query_rows.shape
    q_blocks = query_rows.reshape(blocks, query_count // blocks, head_count, head_dim)
    key_f32 = key_rows.astype(jnp.float32)
    value_f32 = value_rows.astype(jnp.float32)

    def one_block(q_block):
        scores = jnp.einsum("qhd,khd->hqk", q_block.astype(jnp.float32), key_f32) * (head_dim ** -0.5)
        attn_probs = jax.nn.softmax(scores, axis=-1).astype(jnp.bfloat16)
        return jnp.einsum("hqk,khd->qhd", attn_probs.astype(jnp.float32), value_f32).astype(jnp.bfloat16)

    return lax.map(one_block, q_blocks).reshape(query_count, head_count, head_dim)


def transformer_block(hidden, vec_rows, w_qkv, w_o, w_one, w_two, blocks):
    head_count, head_dim = w_qkv.shape[2], w_qkv.shape[3]
    normed = layer_norm(hidden, vec_rows[0], vec_rows[1]).astype(jnp.bfloat16)
    qkv_bias = jnp.stack([vec_rows[4], jnp.zeros_like(vec_rows[4]), vec_rows[5]]).reshape(1, 3, head_count, head_dim)
    qkv_rows = (jnp.einsum("nd,dche->nche", normed.astype(jnp.float32), w_qkv.astype(jnp.float32)) + qkv_bias).astype(jnp.bfloat16)
    attended = attention(qkv_rows[:, 0], qkv_rows[:, 1], qkv_rows[:, 2], blocks)
    residual = (hidden.astype(jnp.float32) + jnp.einsum("nhe,hed->nd", attended.astype(jnp.float32), w_o.astype(jnp.float32)) + vec_rows[6]).astype(jnp.bfloat16)
    normed_mlp = layer_norm(residual, vec_rows[2], vec_rows[3]).astype(jnp.bfloat16)
    mlp_hidden = jax.nn.gelu(jnp.dot(normed_mlp, w_one, preferred_element_type=jnp.float32) + vec_rows[8:12].reshape(-1), approximate=False).astype(jnp.bfloat16)
    return (residual.astype(jnp.float32) + jnp.dot(mlp_hidden, w_two, preferred_element_type=jnp.float32) + vec_rows[7]).astype(jnp.bfloat16)


def run_stack(hidden, vec_stack, wqkv_stack, wo_stack, w1_stack, w2_stack, blocks):
    def layer_step(hidden_state, layer_params):
        vec_rows, w_qkv, w_o, w_one, w_two = layer_params
        return transformer_block(hidden_state, vec_rows, w_qkv, w_o, w_one, w_two, blocks), None

    final_state, _ = lax.scan(layer_step, hidden, (vec_stack, wqkv_stack, wo_stack, w1_stack, w2_stack))
    return final_state


def reference(patches, enc_pos, vis_mask, dec_pos, w_embed, b_embed, enc_vec, enc_wqkv, enc_wo, enc_w1, enc_w2, enc_final, w_dec_in, mask_token, dec_vec, dec_wqkv, dec_wo, dec_w1, dec_w2, dec_final, w_out):
    vis_idx = jnp.nonzero(vis_mask, size=VISIBLE)[0]
    embedded = (jnp.dot(patches[vis_idx], w_embed, preferred_element_type=jnp.float32) + b_embed + enc_pos[vis_idx].astype(jnp.float32)).astype(jnp.bfloat16)
    encoded = run_stack(embedded, enc_vec, enc_wqkv, enc_wo, enc_w1, enc_w2, SHARDS)
    latent = jnp.dot(layer_norm(encoded, enc_final[0], enc_final[1]).astype(jnp.bfloat16), w_dec_in, preferred_element_type=jnp.float32).astype(jnp.bfloat16)
    scattered = jnp.zeros((TOKENS, DEC_WIDTH), jnp.float32).at[vis_idx].set(latent.astype(jnp.float32))
    dec_in = (jnp.where(vis_mask[:, None] == 1, scattered, mask_token.astype(jnp.float32)) + dec_pos.astype(jnp.float32)).astype(jnp.bfloat16)
    decoded = run_stack(dec_in, dec_vec, dec_wqkv, dec_wo, dec_w1, dec_w2, SHARDS)
    return jnp.dot(layer_norm(decoded, dec_final[0], dec_final[1]).astype(jnp.bfloat16), w_out, preferred_element_type=jnp.float32)
```

```python
import functools
import math

import jax
import jax.numpy as jnp
from jax import lax
from jax.experimental import pallas as pl
from jax.experimental.pallas import tpu as pltpu
from jax.sharding import PartitionSpec as P

LN_EPS = 1e-6
MESH = pl.DeviceIdType.MESH
TOKEN_AXES = ("batch", "time", "region")
F32, BF16 = jnp.float32, jnp.bfloat16
NT = (((1,), (1,)), ((), ()))
TN = (((0,), (0,)), ((), ()))
NN = (((1,), (0,)), ((), ()))
LOG2E = 1.4426950408889634
BIG, MID = 66_000_000, 60_000_000
LANES, TOK, ENC, DEC = 128, 256, 1280, 512
PART, HID, CODED, KEYS, ALL = 640, 2560, 640, 2048, 1536


def vm(*shape):
    return pltpu.VMEM(shape, BF16)


def vmf(*shape):
    return pltpu.VMEM(shape, F32)


def mm(lhs, rhs, dims=NN):
    return lax.dot_general(lhs, rhs, dims, preferred_element_type=F32)


def norm(x, gain, shift):
    mean = jnp.mean(x, axis=-1, keepdims=True)
    cen = x - mean
    var = jnp.mean(cen * cen, axis=-1, keepdims=True)
    return cen * lax.rsqrt(var + LN_EPS) * gain + shift


def norm_rows(src, dst, gain, shift, step):
    def body(i, _):
        rows = pl.ds(pl.multiple_of(i * step, step), step)
        dst[rows, :] = norm(src[rows, :].astype(F32), gain, shift).astype(BF16)
        return 0
    lax.fori_loop(0, src.shape[0] // step, body, 0)


def gelu(x):
    return 0.5 * x * (1.0 + lax.erf(x * (0.5 ** 0.5)))


def column(row, lanes):
    wide = jnp.broadcast_to(row, (LANES, row.shape[1])).T
    return jnp.concatenate([wide] * (lanes // LANES), axis=1)


def neighbours():
    time, region = lax.axis_index("time"), lax.axis_index("region")
    mate = {"batch": 0, "time": time, "region": region + 1 - 2 * (region % 2)}
    across = {"batch": 0, "time": time, "region": (region + 2) % 4}
    along = {"batch": 0, "time": 1 - time, "region": region}
    return mate, across, along


def greet(peers):
    barrier = pltpu.get_barrier_semaphore()
    for peer in peers:
        pl.semaphore_signal(barrier, inc=1, device_id=peer, device_id_type=MESH)
    pl.semaphore_wait(barrier, len(peers))


def push(src, dst, send, recv, peer):
    return pltpu.make_async_remote_copy(src_ref=src, dst_ref=dst, send_sem=send, recv_sem=recv, device_id=peer, device_id_type=MESH)


class Gather:
    def __init__(self, src, slots, send, recv):
        self.mate, self.across, self.along = neighbours()
        half = slots.shape[1] // 2
        top, low = pl.ds(0, half), pl.ds(half, half)
        c = lambda i, s, d, peer: push(s, d, send.at[i], recv.at[i], peer)
        self.first = [c(0, src, slots.at[1], self.mate), c(1, src, slots.at[2], self.across), c(2, src, slots.at[4], self.along)]
        self.from_x = [c(3, slots.at[2, top], slots.at[6, top], self.along), c(4, slots.at[2], slots.at[3], self.mate)]
        self.from_y = [c(5, slots.at[4, low], slots.at[6, low], self.across), c(6, slots.at[4], slots.at[5], self.mate)]
        self.last = [c(7, slots.at[6, top], slots.at[7, top], self.mate), c(8, slots.at[6, low], slots.at[7, low], self.mate)]

    def start(self):
        for copy in self.first:
            copy.start()

    def relay(self):
        self.first[1].wait_recv()
        for copy in self.from_x:
            copy.start()
        self.first[2].wait_recv()
        for copy in self.from_y:
            copy.start()

    def relay_last(self):
        self.from_x[0].wait_recv()
        self.last[0].start()
        self.from_y[0].wait_recv()
        self.last[1].start()

    def finish(self):
        for copy in (self.first[0], self.from_x[1], self.from_y[1], *self.last):
            copy.wait_recv()

    def drain(self):
        for copy in (*self.first, *self.from_x, *self.from_y, *self.last):
            copy.wait_send()


def encoder_kernel(patches, enc_pos, mask, dec_pos, b_embed, vec, fin, w_embed, w_qkv, w_o, w_one, w_two, w_dec,
                   z_out, dall,
                   wemb, wqkv, wo, w1, w2, wdec, ebuf, drecv, csum, xrecv, hb, h, a, qkv, att, g, xs, xr, dsrc,
                   wsem, esend, erecv, xsend, xrecvs, gsend, grecv, osem):
    layers = w_qkv.shape[0]
    core = lax.axis_index("region") % 2
    mate, across, along = neighbours()
    width = h.shape[1]
    heads = 8
    dim = qkv.shape[1] // heads
    part = qkv.shape[1]
    hid = w1.shape[2]
    feats = pl.ds(pl.multiple_of(core * part, LANES), part)
    hids = pl.ds(pl.multiple_of(core * hid, LANES), hid)

    load_embed = pltpu.make_async_copy(w_embed, wemb, wsem.at[0])
    load_embed.start()
    greet([mate, across, along])

    mrow = mask[:].astype(F32).astype(BF16)
    tok = mrow.shape[1]
    row_id = lax.broadcasted_iota(jnp.int32, (tok, tok), 0)
    col_id = lax.broadcasted_iota(jnp.int32, (tok, tok), 1)
    upper = (row_id <= col_id).astype(F32).astype(BF16)
    lower = (row_id >= col_id).astype(F32).astype(BF16)
    same = (row_id == col_id).astype(F32).astype(BF16)
    mrows = jnp.broadcast_to(mrow, (LANES, tok))
    rank = mm(mrows, upper)
    slot = lax.broadcasted_iota(jnp.int32, (LANES, tok), 0).astype(F32) + 1.0
    sel_f = jnp.where((rank == slot) & (mrows.astype(F32) > 0.5), 1.0, 0.0)
    sel = sel_f.astype(BF16)
    valid = jnp.sum(sel_f, axis=1, keepdims=True) > 0.5
    code = mm(lower, mrows, NT) * mm(same, mrows, NT)
    dsrc[:, 0:DEC] = dec_pos[:]
    dsrc[:, DEC:PART] = code.astype(BF16)
    picked = mm(sel, patches[:]).astype(BF16)

    load_embed.wait()
    loads = {}
    k = 1
    for l in range(layers):
        for w in range(3):
            loads["qkv", l, w] = pltpu.make_async_copy(w_qkv.at[l, w, feats], wqkv.at[l, w], wsem.at[k + w])
        loads["o", l] = pltpu.make_async_copy(w_o.at[l, feats], wo.at[l], wsem.at[k + 3])
        loads["one", l] = pltpu.make_async_copy(w_one.at[l, :, hids], w1.at[l], wsem.at[k + 4])
        loads["two", l] = pltpu.make_async_copy(w_two.at[l, hids], w2.at[l], wsem.at[k + 5])
        k += 6
    loads["dec"] = pltpu.make_async_copy(w_dec, wdec, wsem.at[k])
    for load in loads.values():
        load.start()

    chunks = width // TOK
    pairs, xs1, ys1, f1, f2 = [], [], [], [], []
    for j in range(chunks):
        pairs.append(push(ebuf.at[j, 1 - core], drecv.at[j], esend.at[0, j], erecv.at[0, j], mate))
        xs1.append(push(csum.at[j], xrecv.at[j], esend.at[1, j], erecv.at[1, j], across))
        ys1.append(push(hb.at[0, core, j], hb.at[1, core, j], esend.at[2, j], erecv.at[2, j], along))
        f1.append(push(hb.at[0, core, j], hb.at[0, core, j], esend.at[3, j], erecv.at[3, j], mate))
        f2.append(push(hb.at[1, core, j], hb.at[1, core, j], esend.at[4, j], erecv.at[4, j], mate))
    for j in range(chunks):
        cols = slice(TOK * j, TOK * (j + 1))
        e = mm(picked, wemb[:, cols]) + b_embed[:, cols] + mm(sel, enc_pos[:, cols])
        e = jnp.where(valid, e, 0.0).astype(BF16)
        ebuf[j, 0] = e[:, :LANES]
        ebuf[j, 1] = e[:, LANES:]
        pairs[j].start()
    for j in range(chunks):
        pairs[j].wait_recv()
        csum[j] = ebuf[j, core] + drecv[j]
        xs1[j].start()
    for j in range(chunks):
        xs1[j].wait_recv()
        hb[0, core, j] = csum[j] + xrecv[j]
        ys1[j].start()
        f1[j].start()
    for j in range(chunks):
        ys1[j].wait_recv()
        f2[j].start()
    in_f1 = [push(hb.at[0, 1 - core, j], hb.at[0, 1 - core, j], esend.at[3, j], erecv.at[3, j], mate) for j in range(chunks)]
    in_f2 = [push(hb.at[1, 1 - core, j], hb.at[1, 1 - core, j], esend.at[4, j], erecv.at[4, j], mate) for j in range(chunks)]
    for j in range(chunks):
        in_f1[j].wait_recv()
        in_f2[j].wait_recv()
    for j in range(chunks):
        for copy in (pairs[j], xs1[j], ys1[j], f1[j], f2[j]):
            copy.wait_send()

    gather = Gather(dsrc, dall, gsend, grecv)
    own = pltpu.make_async_copy(dsrc, dall.at[0], osem.at[0])
    own.start()
    gather.start()

    for t in range(2):
        for half in range(2):
            for j in range(chunks):
                h[LANES * t:LANES * (t + 1), TOK * j + LANES * half:TOK * j + LANES * half + LANES] = hb[t, half, j]

    def exchange(slot):
        return [push(xs.at[slot, j], xr.at[slot, j], xsend.at[slot, j], xrecvs.at[slot, j], mate) for j in range(chunks)]

    for l in range(layers):
        norm_rows(h, a, vec[0, l:l + 1, :], vec[1, l:l + 1, :], 64)
        for w in range(3):
            loads["qkv", l, w].wait()
            r = mm(wqkv[l, w], a[:], NT)
            if w != 1:
                r = r + column(vec[4 if w == 0 else 5, l:l + 1, feats], TOK)
            qkv[w] = r.astype(BF16)
        for hd in range(heads):
            rows = slice(hd * dim, (hd + 1) * dim)
            s = mm(qkv[1, rows], qkv[0, rows], TN) * (dim ** -0.5)
            p = jnp.exp(s - jnp.max(s, axis=0, keepdims=True))
            p = p * (1.0 / jnp.sum(p, axis=0, keepdims=True))
            att[rows, :] = mm(qkv[2, rows], p.astype(BF16)).astype(BF16)
        loads["o", l].wait()
        copies = exchange(0)
        for j in range(chunks):
            if l > 0:
                copies[j].wait_send()
            xs[0, j] = mm(att[:], wo[l, :, TOK * j:TOK * (j + 1)], TN)
            copies[j].start()
        if l == 0:
            gather.relay()
        else:
            gather.relay_last()
        for j in range(chunks):
            cols = slice(TOK * j, TOK * (j + 1))
            copies[j].wait_recv()
            h[:, cols] = (h[:, cols].astype(F32) + (xs[0, j] + xr[0, j]) + vec[6, l:l + 1, cols]).astype(BF16)
        norm_rows(h, a, vec[2, l:l + 1, :], vec[3, l:l + 1, :], 64)
        loads["one", l].wait()
        for j in range(hid // TOK):
            cols = slice(TOK * j, TOK * (j + 1))
            at = (TOK * j) % width
            bias = vec[8 + (hid // width) * core + (TOK * j) // width, l:l + 1, at:at + TOK]
            g[:, cols] = gelu(mm(a[:], w1[l, :, cols]) + bias).astype(BF16)
        loads["two", l].wait()
        copies = exchange(1)
        for j in range(chunks):
            if l > 0:
                copies[j].wait_send()
            xs[1, j] = mm(g[:], w2[l, :, TOK * j:TOK * (j + 1)])
            copies[j].start()
        for j in range(chunks):
            cols = slice(TOK * j, TOK * (j + 1))
            copies[j].wait_recv()
            h[:, cols] = (h[:, cols].astype(F32) + (xs[1, j] + xr[1, j]) + vec[7, l:l + 1, cols]).astype(BF16)
    norm_rows(h, a, fin[0:1, :], fin[1:2, :], 64)
    loads["dec"].wait()
    z_out[:] = mm(a[:], wdec[:]).astype(BF16)
    for slot in range(2):
        for copy in exchange(slot):
            copy.wait_send()
    gather.finish()
    gather.drain()
    own.wait()


def attend(q, kt, vt, att, buf, peak, heads, dim, keys):
    scale = dim ** -0.5 * LOG2E
    tiles = keys // TOK

    def rows_of(hd):
        return pl.ds(pl.multiple_of(hd * dim, dim), dim)

    def step(score_hd, score_slot, hd, slot):
        best = jnp.full((8, TOK), -jnp.inf, F32)
        if hd is not None:
            top = jnp.max(peak[slot], axis=0, keepdims=True) * scale
            total = jnp.zeros((8, TOK), F32)
            out = jnp.zeros((dim, TOK), F32)
        for i in range(tiles):
            cols = slice(TOK * i, TOK * (i + 1))
            s = mm(kt[rows_of(score_hd), cols], q[rows_of(score_hd), :], TN)
            buf[score_slot][cols, :] = s
            best = jnp.maximum(best, jnp.max(s.reshape(32, 8, TOK), axis=0))
            if hd is not None:
                p = jnp.exp2(buf[slot][cols, :] * scale - top)
                total = total + jnp.sum(p.reshape(32, 8, TOK), axis=0)
                out = out + mm(vt[rows_of(hd), cols], p.astype(BF16))
        peak[score_slot] = best
        if hd is not None:
            total = jnp.sum(total, axis=0, keepdims=True)
            att[rows_of(hd), :] = (out * (1.0 / total)).astype(BF16)

    step(0, 0, None, None)

    def body(i, _):
        step(2 * i + 1, 1, 2 * i, 0)
        step(jnp.minimum(2 * i + 2, heads - 1), 0, 2 * i + 1, 1)
        return 0
    lax.fori_loop(0, heads // 2, body, 0)


def block_tail(h, att, a, g, vec, l, wo, w1, w2):
    h[:] = (h[:].astype(F32) + mm(att[:], wo[:], TN) + vec[6, l:l + 1, :]).astype(BF16)
    norm_rows(h, a, vec[2, l:l + 1, :], vec[3, l:l + 1, :], LANES)
    width = h.shape[1]
    for j in range(w1.shape[1] // width):
        cols = slice(width * j, width * (j + 1))
        g[:, cols] = gelu(mm(a[:], w1[:, cols]) + vec[8 + j, l:l + 1, :]).astype(BF16)
    h[:] = (h[:].astype(F32) + mm(g[:], w2[:]) + vec[7, l:l + 1, :]).astype(BF16)


def decoder_loads(l, w_qkv, w_o, w_one, w_two, wqkv, wo, w1, w2, wsem):
    pairs = ((w_qkv, wqkv), (w_o, wo), (w_one, w1), (w_two, w2))
    return [pltpu.make_async_copy(src.at[l], dst, wsem.at[i]) for i, (src, dst) in enumerate(pairs)]


def keys_values(rows, a_rows, cols, wqkv, kt, vt, vbias):
    kt[:, cols] = mm(wqkv[rows:2 * rows, :], a_rows, NT).astype(BF16)
    vt[:, cols] = (mm(wqkv[2 * rows:, :], a_rows, NT) + vbias[:]).astype(BF16)


def first_decoder_kernel(z, dall, token, vec, w_qkv, w_o, w_one, w_two, h_out, a_out,
                         wqkv, wo, w1, w2, h, a, kt, vt, q, att, g, buf0, buf1, peak, vbias, wsem):
    width = h.shape[1]
    loads = decoder_loads(0, w_qkv, w_o, w_one, w_two, wqkv, wo, w1, w2, wsem)
    for load in loads:
        load.start()
    vbias[:] = column(vec[5, 0:1, :], TOK)
    lane = lax.broadcasted_iota(jnp.int32, (TOK, LANES), 1).astype(F32) + 1.0
    loads[0].wait()

    def build(i, _):
        code = dall[i, :, DEC:PART].astype(F32)
        pick = jnp.where(code == lane, 1.0, 0.0).astype(BF16)
        block = jnp.where(i < 4, 0, LANES)
        placed = mm(pick, z[pl.ds(pl.multiple_of(block, LANES), LANES), :])
        seen = code[:, 0:1] > 0.5
        u = (jnp.where(seen, placed, token[:].astype(F32)) + dall[i, :, 0:DEC].astype(F32)).astype(BF16)
        a_rows = norm(u.astype(F32), vec[0, 0:1, :], vec[1, 0:1, :]).astype(BF16)

        @pl.when(i == 0)
        def _():
            h[:] = u
            a[:] = a_rows
        keys_values(width, a_rows, pl.ds(pl.multiple_of(i * TOK, TOK), TOK), wqkv, kt, vt, vbias)
        return 0
    lax.fori_loop(0, 8, build, 0)
    q[:] = (mm(wqkv[0:width, :], a[:], NT) + column(vec[4, 0:1, :], TOK)).astype(BF16)
    attend(q, kt, vt, att, (buf0, buf1), peak, 16, width // 16, KEYS)
    for load in loads[1:]:
        load.wait()
    block_tail(h, att, a, g, vec, 0, wo, w1, w2)
    h_out[:] = h[:]
    norm_rows(h, a_out, vec[0, 1:2, :], vec[1, 1:2, :], LANES)


def last_decoder_kernel(h_in, a_in, vec, fin, w_qkv, w_o, w_one, w_two, y_out,
                        wqkv, wo, w1, w2, h, a, aall, kt, vt, q, att, g, buf0, buf1, peak, vbias, wsem, gsend, grecv):
    width = h.shape[1]
    loads = decoder_loads(1, w_qkv, w_o, w_one, w_two, wqkv, wo, w1, w2, wsem)
    greet(neighbours())
    gather = Gather(a_in, aall, gsend, grecv)
    gather.start()
    for load in loads:
        load.start()
    h[:] = h_in[:]
    vbias[:] = column(vec[5, 1:2, :], TOK)
    loads[0].wait()
    q[:] = (mm(wqkv[0:width, :], a_in[:], NT) + column(vec[4, 1:2, :], TOK)).astype(BF16)
    keys_values(width, a_in[:], slice(0, TOK), wqkv, kt, vt, vbias)
    gather.relay()
    gather.relay_last()
    gather.finish()

    def build(i, _):
        keys_values(width, aall[i], pl.ds(pl.multiple_of(i * TOK, TOK), TOK), wqkv, kt, vt, vbias)
        return 0
    lax.fori_loop(1, 8, build, 0)
    attend(q, kt, vt, att, (buf0, buf1), peak, 16, width // 16, KEYS)
    for load in loads[1:]:
        load.wait()
    block_tail(h, att, a, g, vec, 1, wo, w1, w2)
    norm_rows(h, y_out, fin[0:1, :], fin[1:2, :], LANES)
    gather.drain()


VM = pl.BlockSpec(memory_space=pltpu.VMEM)
HB = pl.BlockSpec(memory_space=pl.ANY)


def decoder_scratch():
    return [
        vm(ALL, DEC), vm(DEC, DEC), vm(DEC, KEYS), vm(KEYS, DEC),
        vm(TOK, DEC), vm(TOK, DEC),
    ], [
        vm(DEC, KEYS), vm(DEC, KEYS), vm(DEC, TOK), vm(DEC, TOK),
        vm(TOK, KEYS), vmf(KEYS, TOK), vmf(KEYS, TOK), vmf(2, 8, TOK),
        vmf(DEC, TOK), pltpu.SemaphoreType.DMA((4,)),
    ]


def solution(mesh):
    def local_step(patches, enc_pos, vis_mask, dec_pos, w_embed, b_embed, enc_vec, enc_wqkv, enc_wo, enc_w1, enc_w2, enc_final, w_dec_in, mask_token, dec_vec, dec_wqkv, dec_wo, dec_w1, dec_w2, dec_final, w_out):
        layers = enc_vec.shape[0]
        evec = jnp.transpose(enc_vec, (1, 0, 2))
        dvec = jnp.transpose(dec_vec, (1, 0, 2))
        ewqkv = jnp.transpose(enc_wqkv, (0, 2, 3, 4, 1)).reshape(layers, 3, ENC, ENC)
        ewo = enc_wo.reshape(layers, ENC, ENC)
        dwqkv = jnp.transpose(dec_wqkv, (0, 2, 3, 4, 1)).reshape(layers, ALL, DEC)
        dwo = dec_wo.reshape(layers, DEC, DEC)
        dma = pltpu.SemaphoreType.DMA
        z, dall = pl.pallas_call(
            encoder_kernel,
            out_shape=(jax.ShapeDtypeStruct((TOK, DEC), BF16), jax.ShapeDtypeStruct((8, TOK, PART), BF16)),
            in_specs=[VM] * 7 + [HB] * 6,
            out_specs=(VM, HB),
            scratch_shapes=[
                vm(ALL, ENC),
                vm(layers, 3, PART, ENC), vm(layers, PART, ENC),
                vm(layers, ENC, HID), vm(layers, HID, ENC), vm(ENC, DEC),
                vm(5, 2, LANES, LANES), vm(5, LANES, LANES), vm(5, LANES, LANES),
                vm(5, LANES, LANES), vm(2, 2, 5, LANES, LANES),
                vm(TOK, ENC), vm(TOK, ENC),
                vm(3, PART, TOK), vm(PART, TOK), vm(TOK, HID),
                vmf(2, 5, TOK, TOK), vmf(2, 5, TOK, TOK), vm(TOK, PART),
                dma((14,)), dma((5, 5)), dma((5, 5)), dma((2, 5)), dma((2, 5)), dma((9,)), dma((9,)), dma((1,)),
            ],
            compiler_params=pltpu.CompilerParams(collective_id=0, has_side_effects=True, vmem_limit_bytes=BIG),
            name="encoder",
        )(patches, enc_pos, vis_mask.reshape(1, -1), dec_pos, b_embed.reshape(1, -1), evec, enc_final, w_embed, ewqkv, ewo, enc_w1, enc_w2, w_dec_in)
        head, tail = decoder_scratch()
        rows = jax.ShapeDtypeStruct((TOK, DEC), BF16)
        h, a = pl.pallas_call(
            first_decoder_kernel,
            out_shape=(rows, rows),
            in_specs=[VM] * 4 + [HB] * 4,
            out_specs=(VM, VM),
            scratch_shapes=head + tail,
            compiler_params=pltpu.CompilerParams(vmem_limit_bytes=MID),
            name="decoder_first",
        )(z, dall, mask_token.reshape(1, -1), dvec, dwqkv, dwo, dec_w1, dec_w2)
        y = pl.pallas_call(
            last_decoder_kernel,
            out_shape=rows,
            in_specs=[VM] * 4 + [HB] * 4,
            out_specs=VM,
            scratch_shapes=head + [vm(8, TOK, DEC)] + tail + [dma((9,)), dma((9,))],
            compiler_params=pltpu.CompilerParams(collective_id=1, has_side_effects=True, vmem_limit_bytes=MID),
            name="decoder_last",
        )(h, a, dvec, dec_final, dwqkv, dwo, dec_w1, dec_w2)
        return jnp.dot(y, w_out, preferred_element_type=F32)

    token_rows = P(TOKEN_AXES, None)
    in_specs = (token_rows, token_rows, P(TOKEN_AXES), token_rows) + (P(),) * 17
    return jax.shard_map(local_step, mesh=mesh, in_specs=in_specs, out_specs=token_rows, check_vma=False)
```

```python
import functools
import math

import jax
import jax.numpy as jnp
from jax import lax
from jax.experimental import pallas as pl
from jax.experimental.pallas import tpu as pltpu
from jax.sharding import PartitionSpec as P

LN_EPS = 1e-6
MESH = pl.DeviceIdType.MESH
TOKEN_AXES = ("batch", "time", "region")
F32, BF16 = jnp.float32, jnp.bfloat16
NT = (((1,), (1,)), ((), ()))
TN = (((0,), (0,)), ((), ()))
NN = (((1,), (0,)), ((), ()))
LOG2E = 1.4426950408889634
BIG, MID = 66_000_000, 60_000_000
LANES, TOK, ENC, DEC = 128, 256, 1280, 512
PART, HID, CODED, KEYS, ALL = 640, 2560, 640, 2048, 1536


def vm(*shape):
    return pltpu.VMEM(shape, BF16)


def vmf(*shape):
    return pltpu.VMEM(shape, F32)


def mm(lhs, rhs, dims=NN):
    return lax.dot_general(lhs, rhs, dims, preferred_element_type=F32)


def norm(x, gain, shift):
    mean = jnp.mean(x, axis=-1, keepdims=True)
    cen = x - mean
    var = jnp.mean(cen * cen, axis=-1, keepdims=True)
    return cen * lax.rsqrt(var + LN_EPS) * gain + shift


def norm_rows(src, dst, gain, shift, step):
    for i in range(src.shape[0] // step):
        rows = slice(i * step, (i + 1) * step)
        dst[rows, :] = norm(src[rows, :].astype(F32), gain, shift).astype(BF16)


def gelu(x):
    return 0.5 * x * (1.0 + lax.erf(x * (0.5 ** 0.5)))


def column(row):
    return jnp.broadcast_to(row, (LANES, row.shape[1])).T


def twice(col):
    return jnp.concatenate([col, col], axis=1)


def neighbours():
    time, region = lax.axis_index("time"), lax.axis_index("region")
    mate = {"batch": 0, "time": time, "region": region + 1 - 2 * (region % 2)}
    across = {"batch": 0, "time": time, "region": (region + 2) % 4}
    along = {"batch": 0, "time": 1 - time, "region": region}
    return mate, across, along


def greet(peers):
    for peer in peers:
        pl.semaphore_signal(pltpu.get_barrier_semaphore(), inc=1, device_id=peer, device_id_type=MESH)


def greeted(peers):
    pl.semaphore_wait(pltpu.get_barrier_semaphore(), len(peers))


def push(src, dst, send, recv, peer):
    return pltpu.make_async_remote_copy(src_ref=src, dst_ref=dst, send_sem=send, recv_sem=recv, device_id=peer, device_id_type=MESH)


class Gather:
    def __init__(self, src, slots, send, recv):
        self.mate, self.across, self.along = neighbours()
        half = slots.shape[1] // 2
        top, low = pl.ds(0, half), pl.ds(half, half)
        c = lambda i, s, d, peer: push(s, d, send.at[i], recv.at[i], peer)
        self.first = [c(0, src, slots.at[1], self.mate), c(1, src, slots.at[2], self.across), c(2, src, slots.at[4], self.along)]
        self.from_x = [c(3, slots.at[2, top], slots.at[6, top], self.along), c(4, slots.at[2], slots.at[3], self.mate)]
        self.from_y = [c(5, slots.at[4, low], slots.at[6, low], self.across), c(6, slots.at[4], slots.at[5], self.mate)]
        self.last = [c(7, slots.at[6, top], slots.at[7, top], self.mate), c(8, slots.at[6, low], slots.at[7, low], self.mate)]

    def start(self):
        for copy in self.first:
            copy.start()

    def relay(self):
        self.first[1].wait_recv()
        for copy in self.from_x:
            copy.start()
        self.first[2].wait_recv()
        for copy in self.from_y:
            copy.start()

    def relay_last(self):
        self.from_x[0].wait_recv()
        self.last[0].start()
        self.from_y[0].wait_recv()
        self.last[1].start()

    def finish(self):
        for copy in (self.first[0], self.from_x[1], self.from_y[1], *self.last):
            copy.wait_recv()

    def drain(self):
        for copy in (*self.first, *self.from_x, *self.from_y, *self.last):
            copy.wait_send()


def encoder_kernel(patches, enc_pos, mask, dec_pos, b_embed, vec, fin, w_embed, w_qkv, w_o, w_one, w_two, w_dec,
                   z_out, dall,
                   wemb, wqkv, wo, w1, w2, wdec, ebuf, drecv, csum, xrecv, hb, h, a, qkv, att, g, xs, xr, dsrc, bcol,
                   wsem, esend, erecv, xsend, xrecvs, gsend, grecv, osem):
    layers = w_qkv.shape[0]
    core = lax.axis_index("region") % 2
    mate, across, along = peers = neighbours()
    width = h.shape[1]
    heads = 8
    part = att.shape[0]
    dim = part // heads
    hid = w1.shape[2]
    feats = pl.ds(pl.multiple_of(core * part, LANES), part)
    hids = pl.ds(pl.multiple_of(core * hid, LANES), hid)
    chunks = width // TOK
    groups = [(0, 1), (2, 3), (4,)]

    load_embed = pltpu.make_async_copy(w_embed, wemb, wsem.at[0])
    load_embed.start()
    greet(peers)

    mrow = mask[:].astype(F32).astype(BF16)
    tok = mrow.shape[1]
    row_id = lax.broadcasted_iota(jnp.int32, (tok, tok), 0)
    col_id = lax.broadcasted_iota(jnp.int32, (tok, tok), 1)
    upper = (row_id <= col_id).astype(F32).astype(BF16)
    lower = (row_id >= col_id).astype(F32).astype(BF16)
    same = (row_id == col_id).astype(F32).astype(BF16)
    mrows = jnp.broadcast_to(mrow, (LANES, tok))
    rank = mm(mrows, upper)
    slot = lax.broadcasted_iota(jnp.int32, (LANES, tok), 0).astype(F32) + 1.0
    sel_f = jnp.where((rank == slot) & (mrows.astype(F32) > 0.5), 1.0, 0.0)
    sel = sel_f.astype(BF16)
    valid = jnp.sum(sel_f, axis=1, keepdims=True) > 0.5
    picked = mm(sel, patches[:]).astype(BF16)

    load_embed.wait()
    loads = {}
    k = 1
    for l in range(layers):
        for w in range(3):
            loads["qkv", l, w] = pltpu.make_async_copy(w_qkv.at[l, w, feats], wqkv.at[l, pl.ds(w * part, part)], wsem.at[k + w])
        loads["o", l] = pltpu.make_async_copy(w_o.at[l, feats], wo.at[l], wsem.at[k + 3])
        loads["one", l] = pltpu.make_async_copy(w_one.at[l, :, hids], w1.at[l], wsem.at[k + 4])
        loads["two", l] = pltpu.make_async_copy(w_two.at[l, hids], w2.at[l], wsem.at[k + 5])
        k += 6
    loads["dec"] = pltpu.make_async_copy(w_dec, wdec, wsem.at[k])
    for load in loads.values():
        load.start()

    pairs, xs1, ys1, f1, f2 = [], [], [], [], []
    for j in range(chunks):
        pairs.append(push(ebuf.at[j, 1 - core], drecv.at[j], esend.at[0, j], erecv.at[0, j], mate))
        xs1.append(push(csum.at[j], xrecv.at[j], esend.at[1, j], erecv.at[1, j], across))
        ys1.append(push(hb.at[0, core, j], hb.at[1, core, j], esend.at[2, j], erecv.at[2, j], along))
        f1.append(push(hb.at[0, core, j], hb.at[0, core, j], esend.at[3, j], erecv.at[3, j], mate))
        f2.append(push(hb.at[1, core, j], hb.at[1, core, j], esend.at[4, j], erecv.at[4, j], mate))
    for group in groups:
        cols = slice(TOK * group[0], TOK * (group[-1] + 1))
        e = mm(picked, wemb[:, cols]) + b_embed[cols].reshape(1, -1) + mm(sel, enc_pos[:, cols])
        e = jnp.where(valid, e, 0.0).astype(BF16)
        for i, j in enumerate(group):
            ebuf[j, 0] = e[:, TOK * i:TOK * i + LANES]
            ebuf[j, 1] = e[:, TOK * i + LANES:TOK * (i + 1)]
        if group[0] == 0:
            greeted(peers)
        for j in group:
            pairs[j].start()
    for j in range(chunks):
        pairs[j].wait_recv()
        csum[j] = ebuf[j, core] + drecv[j]
        xs1[j].start()
    code = mm(lower, mrows, NT) * mm(same, mrows, NT)
    dsrc[:, 0:DEC] = dec_pos[:]
    dsrc[:, DEC:CODED] = code.astype(BF16)
    for l in range(layers):
        bcol[l, 0] = column(vec[4, l:l + 1, feats])
        bcol[l, 1] = column(vec[5, l:l + 1, feats])
    for j in range(chunks):
        xs1[j].wait_recv()
        hb[0, core, j] = csum[j] + xrecv[j]
        ys1[j].start()
        f1[j].start()
    for j in range(chunks):
        ys1[j].wait_recv()
        f2[j].start()
    in_f1 = [push(hb.at[0, 1 - core, j], hb.at[0, 1 - core, j], esend.at[3, j], erecv.at[3, j], mate) for j in range(chunks)]
    in_f2 = [push(hb.at[1, 1 - core, j], hb.at[1, 1 - core, j], esend.at[4, j], erecv.at[4, j], mate) for j in range(chunks)]
    for j in range(chunks):
        in_f1[j].wait_recv()
        in_f2[j].wait_recv()
    for j in range(chunks):
        for copy in (pairs[j], xs1[j], ys1[j], f1[j], f2[j]):
            copy.wait_send()

    gather = Gather(dsrc, dall, gsend, grecv)
    own = pltpu.make_async_copy(dsrc, dall.at[0], osem.at[0])
    own.start()
    gather.start()

    for t in range(2):
        for half in range(2):
            for j in range(chunks):
                h[LANES * t:LANES * (t + 1), TOK * j + LANES * half:TOK * j + LANES * half + LANES] = hb[t, half, j]

    def exchange(slot):
        return [push(xs.at[slot, j], xr.at[slot, j], xsend.at[slot, j], xrecvs.at[slot, j], mate) for j in range(chunks)]

    def partials(slot, l, lhs, weights, dims):
        copies = exchange(slot)
        if l > 0:
            for copy in copies:
                copy.wait_send()
        for group in groups:
            r = mm(lhs[:], weights[l, :, TOK * group[0]:TOK * (group[-1] + 1)], dims)
            for i, j in enumerate(group):
                xs[slot, j] = r[:, TOK * i:TOK * (i + 1)]
            for j in group:
                copies[j].start()
        return copies

    def add_partials(slot, copies, bias):
        for j in range(chunks):
            cols = slice(TOK * j, TOK * (j + 1))
            copies[j].wait_recv()
            h[:, cols] = (h[:, cols].astype(F32) + (xs[slot, j] + xr[slot, j]) + bias[:, cols]).astype(BF16)

    def scores(hd):
        rows = slice(hd * dim, (hd + 1) * dim)
        return mm(qkv[part + hd * dim:part + (hd + 1) * dim, :], qkv[rows, :], TN)

    for l in range(layers):
        norm_rows(h, a, vec[0, l:l + 1, :], vec[1, l:l + 1, :], 64)
        for w in range(3):
            loads["qkv", l, w].wait()
        mid = 3 * part // 2
        low = mm(wqkv[l, :mid], a[:], NT)
        top = mm(wqkv[l, mid:], a[:], NT)
        qkv[:part, :] = (low[:part] + twice(bcol[l, 0])).astype(BF16)
        qkv[part:mid, :] = low[part:].astype(BF16)
        qkv[mid:2 * part, :] = top[:2 * part - mid].astype(BF16)
        qkv[2 * part:, :] = (top[2 * part - mid:] + twice(bcol[l, 1])).astype(BF16)
        scale = dim ** -0.5 * LOG2E
        s = scores(0)
        for hd in range(heads):
            nxt = scores(hd + 1) if hd + 1 < heads else None
            p = jnp.exp2(s * scale - jnp.max(s, axis=0, keepdims=True) * scale)
            total = jnp.sum(p, axis=0, keepdims=True)
            o = mm(qkv[2 * part + hd * dim:2 * part + (hd + 1) * dim, :], p.astype(BF16))
            att[hd * dim:(hd + 1) * dim, :] = (o * (1.0 / total)).astype(BF16)
            s = nxt
        loads["o", l].wait()
        copies = partials(0, l, att, wo, TN)
        if l > 0:
            gather.relay_last()
        add_partials(0, copies, vec[6, l:l + 1, :])
        norm_rows(h, a, vec[2, l:l + 1, :], vec[3, l:l + 1, :], 64)
        loads["one", l].wait()
        for j in range(hid // TOK):
            cols = slice(TOK * j, TOK * (j + 1))
            at = (TOK * j) % width
            bias = vec[8 + (hid // width) * core + (TOK * j) // width, l:l + 1, at:at + TOK]
            g[:, cols] = gelu(mm(a[:], w1[l, :, cols]) + bias).astype(BF16)
        if l == 0:
            gather.relay()
        loads["two", l].wait()
        copies = partials(1, l, g, w2, NN)
        add_partials(1, copies, vec[7, l:l + 1, :])
    norm_rows(h, a, fin[0:1, :], fin[1:2, :], 64)
    loads["dec"].wait()
    z_out[:] = mm(a[:], wdec[:]).astype(BF16)
    for slot in range(2):
        for copy in exchange(slot):
            copy.wait_send()
    gather.finish()
    gather.drain()
    own.wait()


def attend(q, kt, vt, att, buf, peak, state, dim, tiles, first, last, between=None):
    scale = dim ** -0.5 * LOG2E
    heads = att.shape[0] // dim
    tops, sums, outs = state

    def rows_of(hd):
        return pl.ds(pl.multiple_of(hd * dim, dim), dim)

    def step(score_hd, score_slot, hd, slot):
        best = jnp.full((8, TOK), -jnp.inf, F32)
        if hd is not None:
            top = jnp.max(peak[slot], axis=0, keepdims=True)
            if first:
                total = jnp.zeros((8, TOK), F32)
                out = jnp.zeros((dim, TOK), F32)
            else:
                old = tops[hd]
                top = jnp.maximum(old[0:1], top)
                fade = jnp.exp2((old[0:1] - top) * scale)
                total = sums[hd] * fade
                out = outs[rows_of(hd), :] * fade
            base = top * scale
        for i, tile in enumerate(tiles):
            keys, cols = slice(TOK * i, TOK * (i + 1)), slice(TOK * tile, TOK * (tile + 1))
            if score_hd is not None:
                s = mm(kt[rows_of(score_hd), cols], q[rows_of(score_hd), :], TN)
                buf[score_slot][keys, :] = s
                best = jnp.maximum(best, jnp.max(s.reshape(-1, 8, TOK), axis=0))
            if hd is not None:
                p = jnp.exp2(buf[slot][keys, :] * scale - base)
                total = total + jnp.sum(p.reshape(-1, 8, TOK), axis=0)
                out = out + mm(vt[rows_of(hd), cols], p.astype(BF16))
        if score_hd is not None:
            peak[score_slot] = best
        if hd is not None:
            if last:
                total = jnp.sum(total, axis=0, keepdims=True)
                att[rows_of(hd), :] = (out * (1.0 / total)).astype(BF16)
            else:
                tops[hd] = jnp.broadcast_to(top, (8, TOK))
                sums[hd] = total
                outs[rows_of(hd), :] = out

    def body(i, _):
        step(2 * i + 1, 1, 2 * i, 0)
        step(2 * i + 2, 0, 2 * i + 1, 1)
        return 0

    step(0, 0, None, None)
    half = heads // 4
    lax.fori_loop(0, half, body, 0)
    if between:
        between()
    lax.fori_loop(half, heads // 2 - 1, body, 0)
    step(heads - 1, 1, heads - 2, 0)
    step(None, None, heads - 1, 1)


def block_tail(h, att, a, g, vec, l, wo, w1, w2):
    h[:] = (h[:].astype(F32) + mm(att[:], wo[l], TN) + vec[6, l:l + 1, :]).astype(BF16)
    norm_rows(h, a, vec[2, l:l + 1, :], vec[3, l:l + 1, :], LANES)
    width = h.shape[1]
    for j in range(w1.shape[2] // width):
        cols = slice(width * j, width * (j + 1))
        g[:, cols] = gelu(mm(a[:], w1[l, :, cols]) + vec[8 + j, l:l + 1, :]).astype(BF16)
    h[:] = (h[:].astype(F32) + mm(g[:], w2[l]) + vec[7, l:l + 1, :]).astype(BF16)


def decoder_kernel(z, token, vec, fin, dall, w_qkv, w_o, w_one, w_two, y_out,
                   wqkv, wo, w1, w2, dslots, h, a, own, aall, arecv, kt, vt, q, att, g, buf0, buf1, peak, tops, sums, outs, bcol,
                   wsem, dsem, gsend, grecv):
    width = h.shape[1]
    layers = wqkv.shape[0]
    slots = dslots.shape[0]
    peers = neighbours()
    greet(peers)
    blocks = [pltpu.make_async_copy(dall.at[i], dslots.at[i], dsem.at[i]) for i in range(slots)]
    pairs = ((w_qkv, wqkv), (w_o, wo), (w_one, w1), (w_two, w2))
    loads = [[pltpu.make_async_copy(src.at[l], dst.at[l], wsem.at[l, i]) for i, (src, dst) in enumerate(pairs)] for l in range(layers)]
    loads[0][0].start()
    for block in blocks:
        block.start()

    for l in range(layers):
        bcol[l, 0] = column(vec[4, l:l + 1, :])
        bcol[l, 1] = column(vec[5, l:l + 1, :])
    lane = lax.broadcasted_iota(jnp.int32, (TOK, LANES), 1).astype(F32) + 1.0
    buf, state = (buf0, buf1), (tops, sums, outs)

    def queries(l, rows):
        q[:] = (mm(wqkv[l, 0:width, :], rows, NT) + twice(bcol[l, 0])).astype(BF16)

    def keys_values(l, i):
        cols = slice(TOK * i, TOK * (i + 1))
        rows = aall[i] if l == 0 else arecv[i]
        kt[:, cols] = mm(wqkv[l, width:2 * width, :], rows, NT).astype(BF16)
        vt[:, cols] = (mm(wqkv[l, 2 * width:, :], rows, NT) + twice(bcol[l, 1])).astype(BF16)

    def rows_in(i):
        code = dslots[i, :, DEC:CODED].astype(F32)
        pick = jnp.where(code == lane, 1.0, 0.0).astype(BF16)
        block = 0 if i < slots // 2 else LANES
        placed = mm(pick, z[block:block + LANES, :])
        seen = code[:, 0:1] > 0.5
        u = (jnp.where(seen, placed, token[:].astype(F32).reshape(1, -1)) + dslots[i, :, 0:DEC].astype(F32)).astype(BF16)
        if i == 0:
            h[:] = u
        aall[i] = norm(u.astype(F32), vec[0, 0:1, :], vec[1, 0:1, :]).astype(BF16)

    for block in blocks:
        block.wait()
    loads[0][0].wait()
    for load in loads[0][1:] + loads[1]:
        load.start()
    rows_in(0)
    queries(0, aall[0])
    for i in range(slots):
        keys_values(0, i)
        if i + 1 < slots:
            rows_in(i + 1)
    attend(q, kt, vt, att, buf, peak, state, width // 16, range(slots), True, True)
    for load in loads[0][1:]:
        load.wait()
    block_tail(h, att, a, g, vec, 0, wo, w1, w2)
    norm_rows(h, own, vec[0, 1:2, :], vec[1, 1:2, :], LANES)
    greeted(peers)
    gather = Gather(own, arecv, gsend, grecv)
    gather.start()
    arecv[0] = own[:]
    loads[1][0].wait()
    queries(1, own[:])
    keys_values(1, 0)
    gather.first[0].wait_recv()
    keys_values(1, 1)
    attend(q, kt, vt, att, buf, peak, state, width // 16, (0, 1), True, False)
    gather.relay()
    keys_values(1, 2)
    keys_values(1, 4)
    gather.from_x[1].wait_recv()
    keys_values(1, 3)
    gather.from_y[1].wait_recv()
    keys_values(1, 5)
    attend(q, kt, vt, att, buf, peak, state, width // 16, (2, 3, 4, 5), False, False, gather.relay_last)
    keys_values(1, 6)
    for copy in gather.last:
        copy.wait_recv()
    keys_values(1, 7)
    attend(q, kt, vt, att, buf, peak, state, width // 16, (6, 7), False, True)
    for load in loads[1][1:]:
        load.wait()
    block_tail(h, att, a, g, vec, 1, wo, w1, w2)
    norm_rows(h, y_out, fin[0:1, :], fin[1:2, :], LANES)
    gather.drain()


VM = pl.BlockSpec(memory_space=pltpu.VMEM)
HB = pl.BlockSpec(memory_space=pl.ANY)


def solution(mesh):
    def local_step(patches, enc_pos, vis_mask, dec_pos, w_embed, b_embed, enc_vec, enc_wqkv, enc_wo, enc_w1, enc_w2, enc_final, w_dec_in, mask_token, dec_vec, dec_wqkv, dec_wo, dec_w1, dec_w2, dec_final, w_out):
        layers = enc_vec.shape[0]
        evec = jnp.transpose(enc_vec, (1, 0, 2))
        dvec = jnp.transpose(dec_vec, (1, 0, 2))
        ewqkv = jnp.transpose(enc_wqkv, (0, 2, 3, 4, 1)).reshape(layers, 3, ENC, ENC)
        ewo = enc_wo.reshape(layers, ENC, ENC)
        dwqkv = jnp.transpose(dec_wqkv, (0, 2, 3, 4, 1)).reshape(layers, ALL, DEC)
        dwo = dec_wo.reshape(layers, DEC, DEC)
        dma = pltpu.SemaphoreType.DMA
        chunks = ENC // TOK
        piece = (chunks, LANES, LANES)
        z, dall = pl.pallas_call(
            encoder_kernel,
            out_shape=(jax.ShapeDtypeStruct((TOK, DEC), BF16), jax.ShapeDtypeStruct((8, TOK, CODED), BF16)),
            in_specs=[VM] * 7 + [HB] * 6,
            out_specs=(VM, HB),
            scratch_shapes=[
                vm(ALL, ENC),
                vm(layers, 3 * PART, ENC), vm(layers, PART, ENC), vm(layers, ENC, HID), vm(layers, HID, ENC), vm(ENC, DEC),
                vm(chunks, 2, LANES, LANES), vm(*piece), vm(*piece), vm(*piece), vm(2, 2, *piece),
                vm(TOK, ENC), vm(TOK, ENC), vm(3 * PART, TOK), vm(PART, TOK), vm(TOK, HID),
                vmf(2, chunks, TOK, TOK), vmf(2, chunks, TOK, TOK), vm(TOK, CODED), vmf(layers, 2, PART, LANES),
                dma((14,)), dma((chunks, chunks)), dma((chunks, chunks)), dma((2, chunks)), dma((2, chunks)), dma((9,)), dma((9,)), dma((1,)),
            ],
            compiler_params=pltpu.CompilerParams(collective_id=0, has_side_effects=True, vmem_limit_bytes=BIG),
            name="encoder",
        )(patches, enc_pos, vis_mask.reshape(1, -1), dec_pos, b_embed, evec, enc_final, w_embed, ewqkv, ewo, enc_w1, enc_w2, w_dec_in)
        y = pl.pallas_call(
            decoder_kernel,
            out_shape=jax.ShapeDtypeStruct((TOK, DEC), BF16),
            in_specs=[VM] * 4 + [HB] * 5,
            out_specs=VM,
            scratch_shapes=[
                vm(layers, ALL, DEC), vm(layers, DEC, DEC), vm(layers, DEC, KEYS), vm(layers, KEYS, DEC),
                vm(8, TOK, CODED), vm(TOK, DEC), vm(TOK, DEC), vm(TOK, DEC), vm(8, TOK, DEC), vm(8, TOK, DEC),
                vm(DEC, KEYS), vm(DEC, KEYS), vm(DEC, TOK), vm(DEC, TOK), vm(TOK, KEYS),
                vmf(KEYS, TOK), vmf(KEYS, TOK), vmf(2, 8, TOK), vmf(16, 8, TOK), vmf(16, 8, TOK), vmf(DEC, TOK), vmf(layers, 2, DEC, LANES),
                dma((layers, 4)), dma((8,)), dma((9,)), dma((9,)),
            ],
            compiler_params=pltpu.CompilerParams(collective_id=1, has_side_effects=True, vmem_limit_bytes=MID),
            name="decoder",
        )(z, mask_token, dvec, dec_final, dall, dwqkv, dwo, dec_w1, dec_w2)
        return jnp.dot(y, w_out, preferred_element_type=F32)

    token_rows = P(TOKEN_AXES, None)
    in_specs = (token_rows, token_rows, P(TOKEN_AXES), token_rows) + (P(),) * 17
    return jax.shard_map(local_step, mesh=mesh, in_specs=in_specs, out_specs=token_rows, check_vma=False)
```

```python
import functools
import math

import jax
import jax.numpy as jnp
from jax import lax
from jax.experimental import pallas as pl
from jax.experimental.pallas import tpu as pltpu
from jax.sharding import PartitionSpec as P

LN_EPS = 1e-6
MESH = pl.DeviceIdType.MESH
TOKEN_AXES = ("batch", "time", "region")
F32, BF16 = jnp.float32, jnp.bfloat16
NT = (((1,), (1,)), ((), ()))
TN = (((0,), (0,)), ((), ()))
NN = (((1,), (0,)), ((), ()))
LOG2E = 1.4426950408889634
TERMS, WIDE = 3, 16
BIG, MID = 66_000_000, 60_000_000
LANES, TOK, ENC, DEC = 128, 256, 1280, 512
PART, HID, CODED, KEYS, ALL = 640, 2560, 640, 2048, 1536


def vm(*shape):
    return pltpu.VMEM(shape, BF16)


def vmf(*shape):
    return pltpu.VMEM(shape, F32)


def mm(lhs, rhs, dims=NN):
    return lax.dot_general(lhs, rhs, dims, preferred_element_type=F32)


def norm(x, gain, shift):
    mean = jnp.mean(x, axis=-1, keepdims=True)
    cen = x - mean
    var = jnp.mean(cen * cen, axis=-1, keepdims=True)
    return cen * lax.rsqrt(var + LN_EPS) * gain + shift


def norm_rows(src, dst, gain, shift, step):
    for i in range(src.shape[0] // step):
        rows = slice(i * step, (i + 1) * step)
        dst[rows, :] = norm(src[rows, :].astype(F32), gain, shift).astype(BF16)


def gelu(x):
    return 0.5 * x * (1.0 + lax.erf(x * (0.5 ** 0.5)))


def column(row):
    return jnp.broadcast_to(row, (LANES, row.shape[1])).T


def twice(col):
    return jnp.concatenate([col, col], axis=1)


def neighbours():
    time, region = lax.axis_index("time"), lax.axis_index("region")
    mate = {"batch": 0, "time": time, "region": region + 1 - 2 * (region % 2)}
    across = {"batch": 0, "time": time, "region": (region + 2) % 4}
    along = {"batch": 0, "time": 1 - time, "region": region}
    return mate, across, along


def greet(peers):
    for peer in peers:
        pl.semaphore_signal(pltpu.get_barrier_semaphore(), inc=1, device_id=peer, device_id_type=MESH)


def greeted(peers):
    pl.semaphore_wait(pltpu.get_barrier_semaphore(), len(peers))


def push(src, dst, send, recv, peer):
    return pltpu.make_async_remote_copy(src_ref=src, dst_ref=dst, send_sem=send, recv_sem=recv, device_id=peer, device_id_type=MESH)


class Gather:
    def __init__(self, src, slots, send, recv):
        self.mate, self.across, self.along = neighbours()
        half = slots.shape[1] // 2
        top, low = pl.ds(0, half), pl.ds(half, half)
        c = lambda i, s, d, peer: push(s, d, send.at[i], recv.at[i], peer)
        self.first = [c(0, src, slots.at[1], self.mate), c(1, src, slots.at[2], self.across), c(2, src, slots.at[4], self.along)]
        self.from_x = [c(3, slots.at[2, top], slots.at[6, top], self.along), c(4, slots.at[2], slots.at[3], self.mate)]
        self.from_y = [c(5, slots.at[4, low], slots.at[6, low], self.across), c(6, slots.at[4], slots.at[5], self.mate)]
        self.last = [c(7, slots.at[6, top], slots.at[7, top], self.mate), c(8, slots.at[6, low], slots.at[7, low], self.mate)]

    def start(self):
        for copy in self.first:
            copy.start()

    def relay(self):
        self.first[1].wait_recv()
        for copy in self.from_x:
            copy.start()
        self.first[2].wait_recv()
        for copy in self.from_y:
            copy.start()

    def relay_last(self):
        self.from_x[0].wait_recv()
        self.last[0].start()
        self.from_y[0].wait_recv()
        self.last[1].start()

    def finish(self):
        for copy in (self.first[0], self.from_x[1], self.from_y[1], *self.last):
            copy.wait_recv()

    def drain(self):
        for copy in (*self.first, *self.from_x, *self.from_y, *self.last):
            copy.wait_send()


def encoder_kernel(patches, enc_pos, mask, dec_pos, b_embed, vec, fin, w_embed, w_qkv, w_o, w_one, w_two, w_dec,
                   z_out, dall,
                   wemb, wqkv, wo, w1, w2, wdec, vecs, ebuf, drecv, csum, xrecv, hb, h, a, qkv, att, g, xs, xr, dsrc, bcol,
                   wsem, lsem, esend, erecv, xsend, xrecvs, gsend, grecv, osem):
    layers = w_qkv.shape[0]
    core = lax.axis_index("region") % 2
    mate, across, along = peers = neighbours()
    width = h.shape[1]
    heads = 8
    part = att.shape[0]
    dim = part // heads
    hid = w1.shape[2]
    feats = pl.ds(pl.multiple_of(core * part, LANES), part)
    hids = pl.ds(pl.multiple_of(core * hid, LANES), hid)
    chunks = width // TOK
    groups = [(0, 1), (2, 3), (4,)]

    load_embed = pltpu.make_async_copy(w_embed, wemb, wsem.at[0])
    load_embed.start()
    greet(peers)

    mrow = mask[:].astype(F32).astype(BF16)
    tok = mrow.shape[1]
    row_id = lax.broadcasted_iota(jnp.int32, (tok, tok), 0)
    col_id = lax.broadcasted_iota(jnp.int32, (tok, tok), 1)
    upper = (row_id <= col_id).astype(F32).astype(BF16)
    lower = (row_id >= col_id).astype(F32).astype(BF16)
    same = (row_id == col_id).astype(F32).astype(BF16)
    mrows = jnp.broadcast_to(mrow, (LANES, tok))
    rank = mm(mrows, upper)
    slot = lax.broadcasted_iota(jnp.int32, (LANES, tok), 0).astype(F32) + 1.0
    sel_f = jnp.where((rank == slot) & (mrows.astype(F32) > 0.5), 1.0, 0.0)
    sel = sel_f.astype(BF16)
    valid = jnp.sum(sel_f, axis=1, keepdims=True) > 0.5
    picked = mm(sel, patches[:]).astype(BF16)

    load_embed.wait()

    def layer_loads(l):
        qkv_loads = [pltpu.make_async_copy(w_qkv.at[l, w, feats], wqkv.at[l, pl.ds(w * part, part)], lsem.at[l, w]) for w in range(3)]
        return qkv_loads + [
            pltpu.make_async_copy(w_o.at[l, feats], wo.at[l], lsem.at[l, 3]),
            pltpu.make_async_copy(w_one.at[l, :, hids], w1.at[l], lsem.at[l, 4]),
            pltpu.make_async_copy(w_two.at[l, hids], w2.at[l], lsem.at[l, 5]),
        ]

    load_dec = pltpu.make_async_copy(w_dec, wdec, wsem.at[1])
    for l in range(layers):
        for load in layer_loads(l):
            load.start()
    load_dec.start()

    pairs, xs1, ys1, f1, f2 = [], [], [], [], []
    for j in range(chunks):
        pairs.append(push(ebuf.at[j, 1 - core], drecv.at[j], esend.at[0, j], erecv.at[0, j], mate))
        xs1.append(push(csum.at[j], xrecv.at[j], esend.at[1, j], erecv.at[1, j], across))
        ys1.append(push(hb.at[0, core, j], hb.at[1, core, j], esend.at[2, j], erecv.at[2, j], along))
        f1.append(push(hb.at[0, core, j], hb.at[0, core, j], esend.at[3, j], erecv.at[3, j], mate))
        f2.append(push(hb.at[1, core, j], hb.at[1, core, j], esend.at[4, j], erecv.at[4, j], mate))
    for group in groups:
        cols = slice(TOK * group[0], TOK * (group[-1] + 1))
        e = mm(picked, wemb[:, cols]) + b_embed[cols].reshape(1, -1) + mm(sel, enc_pos[:, cols])
        e = jnp.where(valid, e, 0.0).astype(BF16)
        for i, j in enumerate(group):
            ebuf[j, 0] = e[:, TOK * i:TOK * i + LANES]
            ebuf[j, 1] = e[:, TOK * i + LANES:TOK * (i + 1)]
        if group[0] == 0:
            greeted(peers)
        for j in group:
            pairs[j].start()
    for j in range(chunks):
        pairs[j].wait_recv()
        csum[j] = ebuf[j, core] + drecv[j]
        xs1[j].start()
    code = mm(lower, mrows, NT) * mm(same, mrows, NT)
    dsrc[:, 0:DEC] = dec_pos[:]
    dsrc[:, DEC:CODED] = code.astype(BF16)
    for l in range(layers):
        vecs[l] = vec[:, l, :]
        bcol[l, 0] = column(vec[4, l:l + 1, feats])
        bcol[l, 1] = column(vec[5, l:l + 1, feats])
    for j in range(chunks):
        xs1[j].wait_recv()
        hb[0, core, j] = csum[j] + xrecv[j]
        ys1[j].start()
        f1[j].start()
    for j in range(chunks):
        ys1[j].wait_recv()
        f2[j].start()
    in_f1 = [push(hb.at[0, 1 - core, j], hb.at[0, 1 - core, j], esend.at[3, j], erecv.at[3, j], mate) for j in range(chunks)]
    in_f2 = [push(hb.at[1, 1 - core, j], hb.at[1, 1 - core, j], esend.at[4, j], erecv.at[4, j], mate) for j in range(chunks)]
    for j in range(chunks):
        in_f1[j].wait_recv()
        in_f2[j].wait_recv()
    for j in range(chunks):
        for copy in (pairs[j], xs1[j], ys1[j], f1[j], f2[j]):
            copy.wait_send()

    gather = Gather(dsrc, dall, gsend, grecv)
    own = pltpu.make_async_copy(dsrc, dall.at[0], osem.at[0])
    own.start()
    gather.start()

    for t in range(2):
        for half in range(2):
            for j in range(chunks):
                h[LANES * t:LANES * (t + 1), TOK * j + LANES * half:TOK * j + LANES * half + LANES] = hb[t, half, j]

    def exchange(slot):
        return [push(xs.at[slot, j], xr.at[slot, j], xsend.at[slot, j], xrecvs.at[slot, j], mate) for j in range(chunks)]

    def partials(slot, l, lhs, weights, dims):
        copies = exchange(slot)

        @pl.when(l > 0)
        def _():
            for copy in copies:
                copy.wait_send()

        for group in groups:
            r = mm(lhs[:], weights[l, :, TOK * group[0]:TOK * (group[-1] + 1)], dims)
            for i, j in enumerate(group):
                xs[slot, j] = r[:, TOK * i:TOK * (i + 1)]
            for j in group:
                copies[j].start()
        return copies

    def add_partials(slot, copies, bias):
        for j in range(chunks):
            cols = slice(TOK * j, TOK * (j + 1))
            copies[j].wait_recv()
            h[:, cols] = (h[:, cols].astype(F32) + (xs[slot, j] + xr[slot, j]) + bias[:, cols]).astype(BF16)

    def scores(hd):
        rows = slice(hd * dim, (hd + 1) * dim)
        return mm(qkv[part + hd * dim:part + (hd + 1) * dim, :], qkv[rows, :], TN)

    def layer(l, _):
        def row(i):
            return vecs[l, i:i + 1, :]

        *qkv_loads, load_o, load_one, load_two = layer_loads(l)
        norm_rows(h, a, row(0), row(1), 64)
        for load in qkv_loads:
            load.wait()
        mid = 3 * part // 2
        low = mm(wqkv[l, :mid], a[:], NT)
        top = mm(wqkv[l, mid:], a[:], NT)
        qkv[:part, :] = (low[:part] + twice(bcol[l, 0])).astype(BF16)
        qkv[part:mid, :] = low[part:].astype(BF16)
        qkv[mid:2 * part, :] = top[:2 * part - mid].astype(BF16)
        qkv[2 * part:, :] = (top[2 * part - mid:] + twice(bcol[l, 1])).astype(BF16)
        scale = dim ** -0.5 * LOG2E
        s = scores(0)
        for hd in range(heads):
            nxt = scores(hd + 1) if hd + 1 < heads else None
            p = jnp.exp2(s * scale - jnp.max(s, axis=0, keepdims=True) * scale)
            total = jnp.sum(p, axis=0, keepdims=True)
            o = mm(qkv[2 * part + hd * dim:2 * part + (hd + 1) * dim, :], p.astype(BF16))
            att[hd * dim:(hd + 1) * dim, :] = (o * (1.0 / total)).astype(BF16)
            s = nxt
        load_o.wait()
        copies = partials(0, l, att, wo, TN)
        pl.when(l > 0)(gather.relay_last)
        add_partials(0, copies, row(6))
        norm_rows(h, a, row(2), row(3), 64)
        load_one.wait()
        wide_bias = [vecs[l, pl.ds(8 + (hid // width) * core + i, 1), :] for i in range(hid // width)]
        for j in range(hid // TOK):
            cols = slice(TOK * j, TOK * (j + 1))
            at = (TOK * j) % width
            bias = wide_bias[(TOK * j) // width][:, at:at + TOK]
            g[:, cols] = gelu(mm(a[:], w1[l, :, cols]) + bias).astype(BF16)
        pl.when(l == 0)(gather.relay)
        load_two.wait()
        copies = partials(1, l, g, w2, NN)
        add_partials(1, copies, row(7))
        return 0

    lax.fori_loop(0, layers, layer, 0)
    norm_rows(h, a, fin[0:1, :], fin[1:2, :], 64)
    load_dec.wait()
    z_out[:] = mm(a[:], wdec[:]).astype(BF16)
    for slot in range(2):
        for copy in exchange(slot):
            copy.wait_send()
    gather.finish()
    gather.drain()
    own.wait()


def attend(q, kt, vt, att, buf, peak, state, dim, tiles, first, last, between=None):
    deep = TERMS * dim
    tops, sums, outs = state
    crew = max(1, WIDE // len(tiles))
    units = att.shape[0] // dim // crew

    def rows_of(hd, size):
        start = hd * size
        return pl.ds(start if isinstance(start, int) else pl.multiple_of(start, size), size)

    def begin(hd, spot):
        top = jnp.max(peak[spot], axis=0, keepdims=True)
        if first:
            return top, jnp.zeros((8, TOK), F32), jnp.zeros((dim, TOK), F32)
        old = tops[hd]
        top = jnp.maximum(old[0:1], top)
        fade = jnp.exp2(old[0:1] - top)
        return top, sums[hd] * fade, outs[rows_of(hd, dim), :] * fade

    def end(hd, top, total, out):
        if last:
            total = jnp.sum(total, axis=0, keepdims=True)
            att[rows_of(hd, dim), :] = (out * (1.0 / total)).astype(BF16)
        else:
            tops[hd] = jnp.broadcast_to(top, (8, TOK))
            sums[hd] = total
            outs[rows_of(hd, dim), :] = out

    def step(score_unit, score_slot, unit, slot):
        best = [jnp.full((8, TOK), -jnp.inf, F32)] * crew
        if unit is not None:
            runs = [begin(unit * crew + n, slot * crew + n) for n in range(crew)]
        for n in range(crew):
            for i, tile in enumerate(tiles):
                keys = slice(TOK * (n * len(tiles) + i), TOK * (n * len(tiles) + i + 1))
                cols = slice(TOK * tile, TOK * (tile + 1))
                if score_unit is not None:
                    rows = rows_of(score_unit * crew + n, deep)
                    s = mm(kt[rows, cols], q[rows, :], TN)
                    buf[score_slot][keys, :] = s
                    best[n] = jnp.maximum(best[n], jnp.max(s.reshape(-1, 8, TOK), axis=0))
                if unit is not None:
                    top, total, out = runs[n]
                    p = jnp.exp2(buf[slot][keys, :] - top)
                    total = total + jnp.sum(p.reshape(-1, 8, TOK), axis=0)
                    out = out + mm(vt[rows_of(unit * crew + n, dim), cols], p.astype(BF16))
                    runs[n] = top, total, out
        for n in range(crew):
            if score_unit is not None:
                peak[score_slot * crew + n] = best[n]
            if unit is not None:
                end(unit * crew + n, *runs[n])

    def body(i, _):
        step(2 * i + 1, 1, 2 * i, 0)
        step(2 * i + 2, 0, 2 * i + 1, 1)
        return 0

    step(0, 0, None, None)
    half = units // 4
    lax.fori_loop(0, half, body, 0)
    if between:
        between()
    lax.fori_loop(half, units // 2 - 1, body, 0)
    step(units - 1, 1, units - 2, 0)
    step(None, None, units - 1, 1)


def block_tail(h, att, a, g, vec, l, wo, w1, w2, rows):
    h[rows, :] = (h[rows, :].astype(F32) + mm(att[:, rows], wo[l], TN) + vec[6, l:l + 1, :]).astype(BF16)
    a[rows, :] = norm(h[rows, :].astype(F32), vec[2, l:l + 1, :], vec[3, l:l + 1, :]).astype(BF16)
    width = h.shape[1]
    for j in range(w1.shape[2] // width):
        cols = slice(width * j, width * (j + 1))
        g[rows, cols] = gelu(mm(a[rows, :], w1[l, :, cols]) + vec[8 + j, l:l + 1, :]).astype(BF16)
    h[rows, :] = (h[rows, :].astype(F32) + mm(g[rows, :], w2[l]) + vec[7, l:l + 1, :]).astype(BF16)


class Halves:
    def __init__(self, src, tiles, send, recv):
        self.mate, self.across, self.along = neighbours()
        half = tiles.shape[1] // 2
        top, low = pl.ds(0, half), pl.ds(half, half)
        made = []

        def c(s, d, peer):
            made.append(push(s, d, send.at[len(made)], recv.at[len(made)], peer))
            return made[-1]

        self.own = [[c(src.at[r], tiles.at[2 + 2 * n, top], self.across), c(src.at[r], tiles.at[2 + 2 * n, low], self.along),
                     c(src.at[r], tiles.at[1, r], self.mate)] for n, r in enumerate((top, low))]
        self.mates = [[c(tiles.at[2 + 2 * n, r], tiles.at[3 + 2 * n, r], self.mate) for r in (top, low)] for n in range(3)]
        self.corner = [c(tiles.at[2, top], tiles.at[6, top], self.along), c(tiles.at[4, low], tiles.at[6, low], self.across)]
        self.made = made

    def start(self, n):
        for copy in self.own[n]:
            copy.start()

    def relay(self, n):
        for i in range(2):
            self.own[n][i].wait_recv()
        self.corner[n].start()
        for copy in self.mates[n]:
            copy.start()

    def relay_corner(self):
        for n in range(2):
            self.corner[n].wait_recv()
            self.mates[2][n].start()

    def from_mate(self, n):
        for copy in self.mates[n]:
            copy.wait_recv()

    def drain(self):
        for copy in self.made:
            copy.wait_send()


def decoder_kernel(z, token, vec, fin, dall, w_qkv, w_o, w_one, w_two, y_out,
                   wqkv, wo, w1, w2, dslots, h, a, own, aall, arecv, kt, vt, q, att, g, buf0, buf1, peak, tops, sums, outs, bcol,
                   wsem, dsem, gsend, grecv):
    width = h.shape[1]
    layers = wqkv.shape[0]
    slots = dslots.shape[0]
    peers = neighbours()
    greet(peers)
    blocks = [pltpu.make_async_copy(dall.at[i], dslots.at[i], dsem.at[i]) for i in range(slots)]
    pairs = ((w_qkv, wqkv), (w_o, wo), (w_one, w1), (w_two, w2))
    loads = [[pltpu.make_async_copy(src.at[l], dst.at[l], wsem.at[l, i]) for i, (src, dst) in enumerate(pairs)] for l in range(layers)]
    loads[0][0].start()
    for block in blocks:
        block.start()

    for l in range(layers):
        bcol[l, 0] = column(vec[4, l:l + 1, :])
        bcol[l, 1] = column(vec[5, l:l + 1, :])
    lane = lax.broadcasted_iota(jnp.int32, (TOK, LANES), 1).astype(F32) + 1.0
    buf, state = (buf0, buf1), (tops, sums, outs)

    dim = width // 16

    def queries(l, rows):
        rest = (mm(wqkv[l, 0:width, :], rows, NT) + twice(bcol[l, 0])).astype(BF16).astype(F32) * (dim ** -0.5 * LOG2E)
        for t in range(TERMS):
            term = rest.astype(BF16)
            rest = rest - term.astype(F32)
            for hd in range(width // dim):
                q[(TERMS * hd + t) * dim:(TERMS * hd + t + 1) * dim, :] = term[hd * dim:(hd + 1) * dim]

    def keys_values(l, i):
        cols = slice(TOK * i, TOK * (i + 1))
        rows = aall[i] if l == 0 else arecv[i]
        key = mm(wqkv[l, width:2 * width, :], rows, NT).astype(BF16)
        for hd in range(width // dim):
            for t in range(TERMS):
                kt[(TERMS * hd + t) * dim:(TERMS * hd + t + 1) * dim, cols] = key[hd * dim:(hd + 1) * dim]
        vt[:, cols] = (mm(wqkv[l, 2 * width:, :], rows, NT) + twice(bcol[l, 1])).astype(BF16)

    def rows_in(i):
        code = dslots[i, :, DEC:CODED].astype(F32)
        pick = jnp.where(code == lane, 1.0, 0.0).astype(BF16)
        block = 0 if i < slots // 2 else LANES
        placed = mm(pick, z[block:block + LANES, :])
        seen = code[:, 0:1] > 0.5
        u = (jnp.where(seen, placed, token[:].astype(F32).reshape(1, -1)) + dslots[i, :, 0:DEC].astype(F32)).astype(BF16)
        if i == 0:
            h[:] = u
        aall[i] = norm(u.astype(F32), vec[0, 0:1, :], vec[1, 0:1, :]).astype(BF16)

    for block in blocks:
        block.wait()
    loads[0][0].wait()
    for load in loads[0][1:] + loads[1]:
        load.start()
    rows_in(0)
    queries(0, aall[0])
    for i in range(slots):
        keys_values(0, i)
        if i + 1 < slots:
            rows_in(i + 1)
    attend(q, kt, vt, att, buf, peak, state, dim, range(slots), True, True)
    for load in loads[0][1:]:
        load.wait()
    gather = Halves(own, arecv, gsend, grecv)
    ways = (slice(0, LANES), slice(LANES, TOK))
    for n, rows in enumerate(ways):
        block_tail(h, att, a, g, vec, 0, wo, w1, w2, rows)
        own[rows, :] = norm(h[rows, :].astype(F32), vec[0, 1:2, :], vec[1, 1:2, :]).astype(BF16)
        if n == 0:
            greeted(peers)
        gather.start(n)
    arecv[0] = own[:]
    loads[1][0].wait()
    queries(1, own[:])
    keys_values(1, 0)
    for n in range(2):
        gather.own[n][2].wait_recv()
    keys_values(1, 1)
    attend(q, kt, vt, att, buf, peak, state, dim, (0, 1), True, False)
    for n in range(2):
        gather.relay(n)
        keys_values(1, 2 + 2 * n)
        gather.from_mate(n)
        keys_values(1, 3 + 2 * n)
        attend(q, kt, vt, att, buf, peak, state, dim, (2 + 2 * n, 3 + 2 * n), False, False)
    gather.relay_corner()
    keys_values(1, 6)
    gather.from_mate(2)
    keys_values(1, 7)
    attend(q, kt, vt, att, buf, peak, state, dim, (6, 7), False, True)
    for load in loads[1][1:]:
        load.wait()
    block_tail(h, att, a, g, vec, 1, wo, w1, w2, slice(0, TOK))
    norm_rows(h, y_out, fin[0:1, :], fin[1:2, :], LANES)
    gather.drain()


VM = pl.BlockSpec(memory_space=pltpu.VMEM)
HB = pl.BlockSpec(memory_space=pl.ANY)


def solution(mesh):
    def local_step(patches, enc_pos, vis_mask, dec_pos, w_embed, b_embed, enc_vec, enc_wqkv, enc_wo, enc_w1, enc_w2, enc_final, w_dec_in, mask_token, dec_vec, dec_wqkv, dec_wo, dec_w1, dec_w2, dec_final, w_out):
        layers = enc_vec.shape[0]
        evec = jnp.transpose(enc_vec, (1, 0, 2))
        dvec = jnp.transpose(dec_vec, (1, 0, 2))
        ewqkv = jnp.transpose(enc_wqkv, (0, 2, 3, 4, 1)).reshape(layers, 3, ENC, ENC)
        ewo = enc_wo.reshape(layers, ENC, ENC)
        dwqkv = jnp.transpose(dec_wqkv, (0, 2, 3, 4, 1)).reshape(layers, ALL, DEC)
        dwo = dec_wo.reshape(layers, DEC, DEC)
        dma = pltpu.SemaphoreType.DMA
        chunks = ENC // TOK
        piece = (chunks, LANES, LANES)
        z, dall = pl.pallas_call(
            encoder_kernel,
            out_shape=(jax.ShapeDtypeStruct((TOK, DEC), BF16), jax.ShapeDtypeStruct((8, TOK, CODED), BF16)),
            in_specs=[VM] * 7 + [HB] * 6,
            out_specs=(VM, HB),
            scratch_shapes=[
                vm(ALL, ENC),
                vm(layers, 3 * PART, ENC), vm(layers, PART, ENC), vm(layers, ENC, HID), vm(layers, HID, ENC), vm(ENC, DEC), vmf(layers, 12, ENC),
                vm(chunks, 2, LANES, LANES), vm(*piece), vm(*piece), vm(*piece), vm(2, 2, *piece),
                vm(TOK, ENC), vm(TOK, ENC), vm(3 * PART, TOK), vm(PART, TOK), vm(TOK, HID),
                vmf(2, chunks, TOK, TOK), vmf(2, chunks, TOK, TOK), vm(TOK, CODED), vmf(layers, 2, PART, LANES),
                dma((2,)), dma((layers, 6)), dma((chunks, chunks)), dma((chunks, chunks)), dma((2, chunks)), dma((2, chunks)), dma((9,)), dma((9,)), dma((1,)),
            ],
            compiler_params=pltpu.CompilerParams(collective_id=0, has_side_effects=True, vmem_limit_bytes=BIG),
            name="encoder",
        )(patches, enc_pos, vis_mask.reshape(1, -1), dec_pos, b_embed, evec, enc_final, w_embed, ewqkv, ewo, enc_w1, enc_w2, w_dec_in)
        y = pl.pallas_call(
            decoder_kernel,
            out_shape=jax.ShapeDtypeStruct((TOK, DEC), BF16),
            in_specs=[VM] * 4 + [HB] * 5,
            out_specs=VM,
            scratch_shapes=[
                vm(layers, ALL, DEC), vm(layers, DEC, DEC), vm(layers, DEC, KEYS), vm(layers, KEYS, DEC),
                vm(8, TOK, CODED), vm(TOK, DEC), vm(TOK, DEC), vm(TOK, DEC), vm(8, TOK, DEC), vm(8, TOK, DEC),
                vm(TERMS * DEC, KEYS), vm(DEC, KEYS), vm(TERMS * DEC, TOK), vm(DEC, TOK), vm(TOK, KEYS),
                vmf(WIDE * TOK, TOK), vmf(WIDE * TOK, TOK), vmf(WIDE, 8, TOK), vmf(16, 8, TOK), vmf(16, 8, TOK), vmf(DEC, TOK), vmf(layers, 2, DEC, LANES),
                dma((layers, 4)), dma((8,)), dma((14,)), dma((14,)),
            ],
            compiler_params=pltpu.CompilerParams(collective_id=1, has_side_effects=True, vmem_limit_bytes=MID),
            name="decoder",
        )(z, mask_token, dvec, dec_final, dall, dwqkv, dwo, dec_w1, dec_w2)
        return jnp.dot(y, w_out, preferred_element_type=F32)

    token_rows = P(TOKEN_AXES, None)
    in_specs = (token_rows, token_rows, P(TOKEN_AXES), token_rows) + (P(),) * 17
    return jax.shard_map(local_step, mesh=mesh, in_specs=in_specs, out_specs=token_rows, check_vma=False)
```

```python
import functools
import math

import jax
import jax.numpy as jnp
from jax import lax
from jax.experimental import pallas as pl
from jax.experimental.pallas import tpu as pltpu
from jax.sharding import PartitionSpec as P

LN_EPS = 1e-6
MESH = pl.DeviceIdType.MESH
TOKEN_AXES = ("batch", "time", "region")
F32, BF16 = jnp.float32, jnp.bfloat16
NT = (((1,), (1,)), ((), ()))
TN = (((0,), (0,)), ((), ()))
NN = (((1,), (0,)), ((), ()))
LOG2E = 1.4426950408889634
TERMS, WIDE = 3, 16
BIG, MID = 66_000_000, 65_000_000
LANES, TOK, ENC, DEC = 128, 256, 1280, 512
PART, HID, CODED, KEYS, ALL = 640, 2560, 640, 2048, 1536


def vm(*shape):
    return pltpu.VMEM(shape, BF16)


def vmf(*shape):
    return pltpu.VMEM(shape, F32)


def mm(lhs, rhs, dims=NN):
    return lax.dot_general(lhs, rhs, dims, preferred_element_type=F32)


def norm(x, gain, shift):
    mean = jnp.mean(x, axis=-1, keepdims=True)
    cen = x - mean
    var = jnp.mean(cen * cen, axis=-1, keepdims=True)
    return cen * lax.rsqrt(var + LN_EPS) * gain + shift


def norm_rows(src, dst, gain, shift, step):
    for i in range(src.shape[0] // step):
        rows = slice(i * step, (i + 1) * step)
        dst[rows, :] = norm(src[rows, :].astype(F32), gain, shift).astype(BF16)


def gelu(x):
    return 0.5 * x * (1.0 + lax.erf(x * (0.5 ** 0.5)))


def column(row):
    return jnp.broadcast_to(row, (LANES, row.shape[1])).T


def twice(col):
    return jnp.concatenate([col, col], axis=1)


def neighbours():
    time, region = lax.axis_index("time"), lax.axis_index("region")
    mate = {"batch": 0, "time": time, "region": region + 1 - 2 * (region % 2)}
    across = {"batch": 0, "time": time, "region": (region + 2) % 4}
    along = {"batch": 0, "time": 1 - time, "region": region}
    return mate, across, along


def greet(peers):
    for peer in peers:
        pl.semaphore_signal(pltpu.get_barrier_semaphore(), inc=1, device_id=peer, device_id_type=MESH)


def greeted(peers):
    pl.semaphore_wait(pltpu.get_barrier_semaphore(), len(peers))


def push(src, dst, send, recv, peer):
    return pltpu.make_async_remote_copy(src_ref=src, dst_ref=dst, send_sem=send, recv_sem=recv, device_id=peer, device_id_type=MESH)


class Gather:
    def __init__(self, src, slots, send, recv):
        self.mate, self.across, self.along = neighbours()
        half = slots.shape[1] // 2
        top, low = pl.ds(0, half), pl.ds(half, half)
        c = lambda i, s, d, peer: push(s, d, send.at[i], recv.at[i], peer)
        self.first = [c(0, src, slots.at[1], self.mate), c(1, src, slots.at[2], self.across), c(2, src, slots.at[4], self.along)]
        self.from_x = [c(3, slots.at[2, top], slots.at[6, top], self.along), c(4, slots.at[2], slots.at[3], self.mate)]
        self.from_y = [c(5, slots.at[4, low], slots.at[6, low], self.across), c(6, slots.at[4], slots.at[5], self.mate)]
        self.last = [c(7, slots.at[6, top], slots.at[7, top], self.mate), c(8, slots.at[6, low], slots.at[7, low], self.mate)]

    def start(self):
        for copy in self.first:
            copy.start()

    def relay(self):
        self.first[1].wait_recv()
        for copy in self.from_x:
            copy.start()
        self.first[2].wait_recv()
        for copy in self.from_y:
            copy.start()

    def relay_last(self):
        self.from_x[0].wait_recv()
        self.last[0].start()
        self.from_y[0].wait_recv()
        self.last[1].start()

    def finish(self):
        for copy in (self.first[0], self.from_x[1], self.from_y[1], *self.last):
            copy.wait_recv()

    def drain(self):
        for copy in (*self.first, *self.from_x, *self.from_y, *self.last):
            copy.wait_send()


def encoder_kernel(mask, b_embed, patches_in, enc_pos_in, dec_pos, vec_in, fin_in, w_embed, w_qkv, w_o, w_one, w_two, w_dec,
                   z_out, dall,
                   patches, enc_pos, vec, fin, wemb, wqkv, wo, w1, w2, wdec, vecs, ebuf, drecv, csum, xrecv, hb, h, a, low_a, qkv, att, peer_att, acc, g, dsrc, bcol,
                   wsem, esem, lsem, esend, erecv, xsend, xrecvs, gsend, grecv, osem):
    layers = w_qkv.shape[0]
    core = lax.axis_index("region") % 2
    mate, across, along = peers = neighbours()
    width = h.shape[1]
    heads = 8
    part = att.shape[0]
    dim = part // heads
    feats = pl.ds(pl.multiple_of(core * part, LANES), part)
    other_feats = pl.ds(pl.multiple_of((1 - core) * part, LANES), part)
    mine = pl.ds(pl.multiple_of(core * LANES, LANES), LANES)
    theirs = pl.ds(pl.multiple_of((1 - core) * LANES, LANES), LANES)
    chunks = width // TOK
    groups = [(0, 1), (2, 3), (4,)]

    spans = [slice(TOK * group[0], TOK * (group[-1] + 1)) for group in groups]
    load_patches = pltpu.make_async_copy(patches_in, patches, wsem.at[2])
    load_pos = pltpu.make_async_copy(enc_pos_in, enc_pos, wsem.at[3])
    load_embed = [pltpu.make_async_copy(w_embed.at[:, span], wemb.at[:, span], esem.at[i]) for i, span in enumerate(spans)]
    late = [pltpu.make_async_copy(vec_in, vec, wsem.at[4]), pltpu.make_async_copy(fin_in, fin, wsem.at[5]),
            pltpu.make_async_copy(dec_pos, dsrc.at[:, pl.ds(0, DEC)], wsem.at[0])]
    for load in (load_patches, load_embed[0], load_pos, *load_embed[1:], *late):
        load.start()
    greet(peers)

    mrow = mask[:].astype(F32).astype(BF16)
    tok = mrow.shape[1]
    row_id = lax.broadcasted_iota(jnp.int32, (tok, tok), 0)
    col_id = lax.broadcasted_iota(jnp.int32, (tok, tok), 1)
    upper = (row_id <= col_id).astype(F32).astype(BF16)
    lower = (row_id >= col_id).astype(F32).astype(BF16)
    same = (row_id == col_id).astype(F32).astype(BF16)
    mrows = jnp.broadcast_to(mrow, (LANES, tok))
    rank = mm(mrows, upper)
    slot = lax.broadcasted_iota(jnp.int32, (LANES, tok), 0).astype(F32) + 1.0
    sel_f = jnp.where((rank == slot) & (mrows.astype(F32) > 0.5), 1.0, 0.0)
    sel = sel_f.astype(BF16)
    valid = jnp.sum(sel_f, axis=1, keepdims=True) > 0.5
    load_patches.wait()
    picked = mm(sel, patches[:]).astype(BF16)

    def layer_loads(l):
        qkv_loads = [pltpu.make_async_copy(w_qkv.at[l, w, feats], wqkv.at[pl.ds(w * part, part)], lsem.at[l, w]) for w in range(3)]
        return qkv_loads + [
            pltpu.make_async_copy(w_o.at[l], wo, lsem.at[l, 3]),
            pltpu.make_async_copy(w_one.at[l], w1, lsem.at[l, 4]),
            pltpu.make_async_copy(w_two.at[l], w2, lsem.at[l, 5]),
        ]

    load_dec = pltpu.make_async_copy(w_dec, wdec, wsem.at[1])

    pairs, xs1, ys1, f1, f2 = [], [], [], [], []
    for j in range(chunks):
        pairs.append(push(ebuf.at[j, 1 - core], drecv.at[j], esend.at[0, j], erecv.at[0, j], mate))
        xs1.append(push(csum.at[j], xrecv.at[j], esend.at[1, j], erecv.at[1, j], across))
        ys1.append(push(hb.at[0, core, j], hb.at[1, core, j], esend.at[2, j], erecv.at[2, j], along))
        f1.append(push(hb.at[0, core, j], hb.at[0, core, j], esend.at[3, j], erecv.at[3, j], mate))
        f2.append(push(hb.at[1, core, j], hb.at[1, core, j], esend.at[4, j], erecv.at[4, j], mate))
    for n, group in enumerate(groups):
        cols = spans[n]
        load_embed[n].wait()
        if n == 0:
            load_pos.wait()
        e = mm(picked, wemb[:, cols]) + b_embed[cols].reshape(1, -1) + mm(sel, enc_pos[:, cols])
        e = jnp.where(valid, e, 0.0).astype(BF16)
        for i, j in enumerate(group):
            ebuf[j, 0] = e[:, TOK * i:TOK * i + LANES]
            ebuf[j, 1] = e[:, TOK * i + LANES:TOK * (i + 1)]
        if group[0] == 0:
            greeted(peers)
        for j in group:
            pairs[j].start()
    for load in layer_loads(0):
        load.start()
    for j in range(chunks):
        pairs[j].wait_recv()
        csum[j] = ebuf[j, core] + drecv[j]
        xs1[j].start()
    code = mm(lower, mrows, NT) * mm(same, mrows, NT)
    dsrc[:, DEC:CODED] = code.astype(BF16)
    for load in late:
        load.wait()
    vecs[layers, 0:2, :] = fin[:]
    for l in range(layers):
        vecs[l] = vec[:, l, :]
        bcol[l, 0] = column(vec[4, l:l + 1, feats])
        bcol[l, 1] = column(vec[5, l:l + 1, feats])
    for j in range(chunks):
        xs1[j].wait_recv()
        hb[0, core, j] = csum[j] + xrecv[j]
        ys1[j].start()
        f1[j].start()
    for j in range(chunks):
        ys1[j].wait_recv()
        f2[j].start()
    in_f1 = [push(hb.at[0, 1 - core, j], hb.at[0, 1 - core, j], esend.at[3, j], erecv.at[3, j], mate) for j in range(chunks)]
    in_f2 = [push(hb.at[1, 1 - core, j], hb.at[1, 1 - core, j], esend.at[4, j], erecv.at[4, j], mate) for j in range(chunks)]
    for j in range(chunks):
        in_f1[j].wait_recv()
        in_f2[j].wait_recv()
    for j in range(chunks):
        for copy in (pairs[j], xs1[j], ys1[j], f1[j], f2[j]):
            copy.wait_send()

    gather = Gather(dsrc, dall, gsend, grecv)
    own = pltpu.make_async_copy(dsrc, dall.at[0], osem.at[0])
    own.start()
    gather.start()

    for t in range(2):
        for half in range(2):
            for j in range(chunks):
                h[LANES * t:LANES * (t + 1), TOK * j + LANES * half:TOK * j + LANES * half + LANES] = hb[t, half, j]

    half_att = part // 2
    send_att = [push(att.at[pl.ds(i * half_att, half_att), theirs], peer_att.at[pl.ds(i * half_att, half_att)], xsend.at[2 + i], xrecvs.at[2 + i], mate)
                for i in range(2)]
    send_rows = push(a.at[mine], a.at[mine], xsend.at[1], xrecvs.at[1], mate)
    get_rows = push(a.at[theirs], a.at[theirs], xsend.at[1], xrecvs.at[1], mate)

    def scores(hd):
        rows = slice(hd * dim, (hd + 1) * dim)
        return mm(qkv[part + hd * dim:part + (hd + 1) * dim, :], qkv[rows, :], TN)

    def layer(l, _):
        def row(i):
            return vecs[l, i:i + 1, :]

        *qkv_loads, load_o, load_one, load_two = layer_loads(l)
        for load in qkv_loads:
            load.wait()
        mid = 3 * part // 2
        low = mm(wqkv[:mid, :], a[:], NT)
        top = mm(wqkv[mid:, :], a[:], NT)
        qkv[:part, :] = (low[:part] + twice(bcol[l, 0])).astype(BF16)
        qkv[part:mid, :] = low[part:].astype(BF16)
        qkv[mid:2 * part, :] = top[:2 * part - mid].astype(BF16)
        qkv[2 * part:, :] = (top[2 * part - mid:] + twice(bcol[l, 1])).astype(BF16)
        ahead = layer_loads(layers - 1)

        @pl.when(l == 0)
        def _():
            for load in (*ahead[:3], load_dec):
                load.start()

        scale = dim ** -0.5 * LOG2E
        s = scores(0)
        for hd in range(heads):
            nxt = scores(hd + 1) if hd + 1 < heads else None
            p = jnp.exp2(s * scale - jnp.max(s, axis=0, keepdims=True) * scale)
            total = jnp.sum(p, axis=0, keepdims=True)
            o = mm(qkv[2 * part + hd * dim:2 * part + (hd + 1) * dim, :], p.astype(BF16))
            att[hd * dim:(hd + 1) * dim, :] = (o * (1.0 / total)).astype(BF16)
            s = nxt
            if hd + 1 == heads // 2:
                send_att[0].start()
        send_att[1].start()
        load_o.wait()
        acc[:] = mm(att[:, mine], wo[feats, :], TN)
        pl.when(l > 0)(gather.relay_last)
        for copy in send_att:
            copy.wait_recv()
        r = acc[:] + mm(peer_att[:], wo[other_feats, :], TN)
        rows = (h[mine, :].astype(F32) + r + row(6)).astype(BF16)
        h[mine, :] = rows
        low_a[:] = norm(rows.astype(F32), row(2), row(3)).astype(BF16)
        for copy in send_att:
            copy.wait_send()
        pl.when(l == 0)(ahead[3].start)
        load_one.wait()
        for j in range(g.shape[1] // TOK):
            cols = slice(TOK * j, TOK * (j + 1))
            at = (TOK * j) % width
            bias = row(8 + (TOK * j) // width)[:, at:at + TOK]
            g[:, cols] = gelu(mm(low_a[:], w1[:, cols]) + bias).astype(BF16)
        pl.when(l == 0)(ahead[4].start)
        pl.when(l == 0)(gather.relay)
        load_two.wait()
        rows = (h[mine, :].astype(F32) + mm(g[:], w2[:]) + row(7)).astype(BF16)
        h[mine, :] = rows
        pl.when(l == 0)(ahead[5].start)
        a[mine, :] = norm(rows.astype(F32), vecs[l + 1, 0:1, :], vecs[l + 1, 1:2, :]).astype(BF16)
        send_rows.start()
        get_rows.wait_recv()
        send_rows.wait_send()
        return 0

    norm_rows(h, a, vecs[0, 0:1, :], vecs[0, 1:2, :], 64)
    lax.fori_loop(0, layers, layer, 0)
    load_dec.wait()
    z_out[:] = mm(a[:], wdec[:]).astype(BF16)
    gather.finish()
    gather.drain()
    own.wait()


def attend(q, kt, vt, att, buf, peak, state, dim, tiles, first, last, between=None):
    deep = TERMS * dim
    tops, sums, outs = state
    crew = max(1, WIDE // len(tiles))
    units = att.shape[0] // dim // crew

    def rows_of(hd, size):
        start = hd * size
        return pl.ds(start if isinstance(start, int) else pl.multiple_of(start, size), size)

    def begin(hd, spot):
        top = jnp.max(peak[spot], axis=0, keepdims=True)
        if first:
            return top, jnp.zeros((8, TOK), F32), jnp.zeros((dim, TOK), F32)
        old = tops[hd]
        top = jnp.maximum(old[0:1], top)
        fade = jnp.exp2(old[0:1] - top)
        return top, sums[hd] * fade, outs[rows_of(hd, dim), :] * fade

    def end(hd, top, total, out):
        if last:
            total = jnp.sum(total, axis=0, keepdims=True)
            att[rows_of(hd, dim), :] = (out * (1.0 / total)).astype(BF16)
        else:
            tops[hd] = jnp.broadcast_to(top, (8, TOK))
            sums[hd] = total
            outs[rows_of(hd, dim), :] = out

    def step(score_unit, score_slot, unit, slot):
        best = [jnp.full((8, TOK), -jnp.inf, F32)] * crew
        if unit is not None:
            runs = [begin(unit * crew + n, slot * crew + n) for n in range(crew)]
        for n in range(crew):
            for i, tile in enumerate(tiles):
                keys = slice(TOK * (n * len(tiles) + i), TOK * (n * len(tiles) + i + 1))
                cols = slice(TOK * tile, TOK * (tile + 1))
                if score_unit is not None:
                    rows = rows_of(score_unit * crew + n, deep)
                    s = mm(kt[rows, cols], q[rows, :], TN)
                    buf[score_slot][keys, :] = s
                    best[n] = jnp.maximum(best[n], jnp.max(s.reshape(-1, 8, TOK), axis=0))
                if unit is not None:
                    top, total, out = runs[n]
                    p = jnp.exp2(buf[slot][keys, :] - top)
                    total = total + jnp.sum(p.reshape(-1, 8, TOK), axis=0)
                    out = out + mm(vt[rows_of(unit * crew + n, dim), cols], p.astype(BF16))
                    runs[n] = top, total, out
        for n in range(crew):
            if score_unit is not None:
                peak[score_slot * crew + n] = best[n]
            if unit is not None:
                end(unit * crew + n, *runs[n])

    def body(i, _):
        step(2 * i + 1, 1, 2 * i, 0)
        step(2 * i + 2, 0, 2 * i + 1, 1)
        return 0

    step(0, 0, None, None)
    half = units // 4
    lax.fori_loop(0, half, body, 0)
    if between:
        between()
    lax.fori_loop(half, units // 2 - 1, body, 0)
    step(units - 1, 1, units - 2, 0)
    step(None, None, units - 1, 1)


def block_tail(h, att, a, g, vec, l, wo, w1, w2, rows):
    h[rows, :] = (h[rows, :].astype(F32) + mm(att[:, rows], wo[l], TN) + vec[6, l:l + 1, :]).astype(BF16)
    a[rows, :] = norm(h[rows, :].astype(F32), vec[2, l:l + 1, :], vec[3, l:l + 1, :]).astype(BF16)
    width = h.shape[1]
    for j in range(w1.shape[2] // width):
        cols = slice(width * j, width * (j + 1))
        g[rows, cols] = gelu(mm(a[rows, :], w1[l, :, cols]) + vec[8 + j, l:l + 1, :]).astype(BF16)
    h[rows, :] = (h[rows, :].astype(F32) + mm(g[rows, :], w2[l]) + vec[7, l:l + 1, :]).astype(BF16)


class Halves:
    def __init__(self, src, tiles, send, recv):
        self.mate, self.across, self.along = neighbours()
        half = tiles.shape[1] // 2
        top, low = pl.ds(0, half), pl.ds(half, half)
        made = []

        def c(s, d, peer):
            made.append(push(s, d, send.at[len(made)], recv.at[len(made)], peer))
            return made[-1]

        self.own = [[c(src.at[r], tiles.at[2 + 2 * n, top], self.across), c(src.at[r], tiles.at[2 + 2 * n, low], self.along),
                     c(src.at[r], tiles.at[1, r], self.mate)] for n, r in enumerate((top, low))]
        self.mates = [[c(tiles.at[2 + 2 * n, r], tiles.at[3 + 2 * n, r], self.mate) for r in (top, low)] for n in range(3)]
        self.corner = [c(tiles.at[2, top], tiles.at[6, top], self.along), c(tiles.at[4, low], tiles.at[6, low], self.across)]
        self.made = made

    def start(self, n):
        for copy in self.own[n]:
            copy.start()

    def relay(self, n):
        for i in range(2):
            self.own[n][i].wait_recv()
        self.corner[n].start()
        for copy in self.mates[n]:
            copy.start()

    def relay_corner(self):
        for n in range(2):
            self.corner[n].wait_recv()
            self.mates[2][n].start()

    def from_mate(self, n):
        for copy in self.mates[n]:
            copy.wait_recv()

    def drain(self):
        for copy in self.made:
            copy.wait_send()


def decoder_kernel(token, vec, fin, z_in, dall, w_qkv, w_o, w_one, w_two, y_out,
                   wqkv, wo, w1, w2, z, dslots, h, a, own, aall, arecv, kt, vt, q, att, g, buf0, buf1, peak, tops, sums, outs, bcol,
                   wsem, dsem, gsend, grecv):
    width = h.shape[1]
    layers = wqkv.shape[0]
    slots = dslots.shape[0]
    peers = neighbours()
    greet(peers)
    blocks = [pltpu.make_async_copy(dall.at[i], dslots.at[i], dsem.at[i]) for i in range(slots)]
    pairs = ((w_qkv, wqkv), (w_o, wo), (w_one, w1), (w_two, w2))
    loads = [[pltpu.make_async_copy(src.at[l], dst.at[l], wsem.at[l, i]) for i, (src, dst) in enumerate(pairs)] for l in range(layers)]
    blocks.append(pltpu.make_async_copy(z_in, z, dsem.at[slots]))
    loads[0][0].start()
    for block in reversed(blocks):
        block.start()

    for l in range(layers):
        bcol[l, 0] = column(vec[4, l:l + 1, :])
        bcol[l, 1] = column(vec[5, l:l + 1, :])
    lane = lax.broadcasted_iota(jnp.int32, (TOK, LANES), 1).astype(F32) + 1.0
    buf, state = (buf0, buf1), (tops, sums, outs)

    dim = width // 16

    def queries(l, rows):
        rest = (mm(wqkv[l, 0:width, :], rows, NT) + twice(bcol[l, 0])).astype(BF16).astype(F32) * (dim ** -0.5 * LOG2E)
        for t in range(TERMS):
            term = rest.astype(BF16)
            rest = rest - term.astype(F32)
            for hd in range(width // dim):
                q[(TERMS * hd + t) * dim:(TERMS * hd + t + 1) * dim, :] = term[hd * dim:(hd + 1) * dim]

    def keys_values(l, i):
        cols = slice(TOK * i, TOK * (i + 1))
        rows = aall[i] if l == 0 else arecv[i]
        key = mm(wqkv[l, width:2 * width, :], rows, NT).astype(BF16)
        for hd in range(width // dim):
            for t in range(TERMS):
                kt[(TERMS * hd + t) * dim:(TERMS * hd + t + 1) * dim, cols] = key[hd * dim:(hd + 1) * dim]
        vt[:, cols] = (mm(wqkv[l, 2 * width:, :], rows, NT) + twice(bcol[l, 1])).astype(BF16)

    def rows_in(i):
        code = dslots[i, :, DEC:CODED].astype(F32)
        pick = jnp.where(code == lane, 1.0, 0.0).astype(BF16)
        block = 0 if i < slots // 2 else LANES
        placed = mm(pick, z[block:block + LANES, :])
        seen = code[:, 0:1] > 0.5
        u = (jnp.where(seen, placed, token[:].astype(F32).reshape(1, -1)) + dslots[i, :, 0:DEC].astype(F32)).astype(BF16)
        if i == 0:
            h[:] = u
        aall[i] = norm(u.astype(F32), vec[0, 0:1, :], vec[1, 0:1, :]).astype(BF16)

    for block in blocks:
        block.wait()
    loads[0][0].wait()
    for load in loads[0][1:] + loads[1]:
        load.start()
    rows_in(0)
    queries(0, aall[0])
    for i in range(slots):
        keys_values(0, i)
        if i + 1 < slots:
            rows_in(i + 1)
    attend(q, kt, vt, att, buf, peak, state, dim, range(slots), True, True)
    for load in loads[0][1:]:
        load.wait()
    gather = Halves(own, arecv, gsend, grecv)
    ways = (slice(0, LANES), slice(LANES, TOK))
    for n, rows in enumerate(ways):
        block_tail(h, att, a, g, vec, 0, wo, w1, w2, rows)
        own[rows, :] = norm(h[rows, :].astype(F32), vec[0, 1:2, :], vec[1, 1:2, :]).astype(BF16)
        if n == 0:
            greeted(peers)
        gather.start(n)
    arecv[0] = own[:]
    loads[1][0].wait()
    queries(1, own[:])
    keys_values(1, 0)
    for n in range(2):
        gather.own[n][2].wait_recv()
    keys_values(1, 1)
    attend(q, kt, vt, att, buf, peak, state, dim, (0, 1), True, False)
    for n in range(2):
        gather.relay(n)
        keys_values(1, 2 + 2 * n)
        gather.from_mate(n)
        keys_values(1, 3 + 2 * n)
        attend(q, kt, vt, att, buf, peak, state, dim, (2 + 2 * n, 3 + 2 * n), False, False)
    gather.relay_corner()
    keys_values(1, 6)
    gather.from_mate(2)
    keys_values(1, 7)
    attend(q, kt, vt, att, buf, peak, state, dim, (6, 7), False, True)
    for load in loads[1][1:]:
        load.wait()
    block_tail(h, att, a, g, vec, 1, wo, w1, w2, slice(0, TOK))
    norm_rows(h, y_out, fin[0:1, :], fin[1:2, :], LANES)
    gather.drain()


VM = pl.BlockSpec(memory_space=pltpu.VMEM)
HB = pl.BlockSpec(memory_space=pl.ANY)
HBM = pl.BlockSpec(memory_space=pltpu.HBM)


def solution(mesh):
    def local_step(patches, enc_pos, vis_mask, dec_pos, w_embed, b_embed, enc_vec, enc_wqkv, enc_wo, enc_w1, enc_w2, enc_final, w_dec_in, mask_token, dec_vec, dec_wqkv, dec_wo, dec_w1, dec_w2, dec_final, w_out):
        layers = enc_vec.shape[0]
        evec = jnp.transpose(enc_vec, (1, 0, 2))
        dvec = jnp.transpose(dec_vec, (1, 0, 2))
        ewqkv = jnp.transpose(enc_wqkv, (0, 2, 3, 4, 1)).reshape(layers, 3, ENC, ENC)
        ewo = enc_wo.reshape(layers, ENC, ENC)
        dwqkv = jnp.transpose(dec_wqkv, (0, 2, 3, 4, 1)).reshape(layers, ALL, DEC)
        dwo = dec_wo.reshape(layers, DEC, DEC)
        dma = pltpu.SemaphoreType.DMA
        chunks = ENC // TOK
        piece = (chunks, LANES, LANES)
        z, dall = pl.pallas_call(
            encoder_kernel,
            out_shape=(jax.ShapeDtypeStruct((TOK, DEC), BF16), jax.ShapeDtypeStruct((8, TOK, CODED), BF16)),
            in_specs=[VM] * 2 + [HB] * 11,
            out_specs=(VM, HB),
            scratch_shapes=[
                vm(TOK, ALL), vm(TOK, ENC), vmf(12, layers, ENC), vmf(2, ENC), vm(ALL, ENC),
                vm(3 * PART, ENC), vm(ENC, ENC), vm(ENC, 2 * HID), vm(2 * HID, ENC), vm(ENC, DEC), vmf(layers + 1, 12, ENC),
                vm(chunks, 2, LANES, LANES), vm(*piece), vm(*piece), vm(*piece), vm(2, 2, *piece),
                vm(TOK, ENC), vm(TOK, ENC), vm(LANES, ENC), vm(3 * PART, TOK), vm(PART, TOK), vm(PART, LANES), vmf(LANES, ENC), vm(LANES, 2 * HID),
                vm(TOK, CODED), vmf(layers, 2, PART, LANES),
                dma((6,)), dma((chunks,)), dma((layers, 6)), dma((chunks, chunks)), dma((chunks, chunks)), dma((4,)), dma((4,)), dma((9,)), dma((9,)), dma((1,)),
            ],
            compiler_params=pltpu.CompilerParams(collective_id=0, has_side_effects=True, vmem_limit_bytes=BIG),
            name="encoder",
        )(vis_mask.reshape(1, -1), b_embed, patches, enc_pos, dec_pos, evec, enc_final, w_embed, ewqkv, ewo, enc_w1, enc_w2, w_dec_in)
        y = pl.pallas_call(
            decoder_kernel,
            out_shape=jax.ShapeDtypeStruct((TOK, DEC), BF16),
            in_specs=[VM] * 3 + [HBM] * 2 + [HB] * 4,
            out_specs=VM,
            scratch_shapes=[
                vm(layers, ALL, DEC), vm(layers, DEC, DEC), vm(layers, DEC, KEYS), vm(layers, KEYS, DEC),
                vm(TOK, DEC), vm(8, TOK, CODED), vm(TOK, DEC), vm(TOK, DEC), vm(TOK, DEC), vm(8, TOK, DEC), vm(8, TOK, DEC),
                vm(TERMS * DEC, KEYS), vm(DEC, KEYS), vm(TERMS * DEC, TOK), vm(DEC, TOK), vm(TOK, KEYS),
                vmf(WIDE * TOK, TOK), vmf(WIDE * TOK, TOK), vmf(WIDE, 8, TOK), vmf(16, 8, TOK), vmf(16, 8, TOK), vmf(DEC, TOK), vmf(layers, 2, DEC, LANES),
                dma((layers, 4)), dma((9,)), dma((14,)), dma((14,)),
            ],
            compiler_params=pltpu.CompilerParams(collective_id=1, has_side_effects=True, vmem_limit_bytes=MID),
            name="decoder",
        )(mask_token, dvec, dec_final, z, dall, dwqkv, dwo, dec_w1, dec_w2)
        return jnp.dot(y, w_out, preferred_element_type=F32)

    token_rows = P(TOKEN_AXES, None)
    in_specs = (token_rows, token_rows, P(TOKEN_AXES), token_rows) + (P(),) * 17
    return jax.shard_map(local_step, mesh=mesh, in_specs=in_specs, out_specs=token_rows, check_vma=False)
```

```python
import functools
import math

import jax
import jax.numpy as jnp
from jax import lax
from jax.experimental import pallas as pl
from jax.experimental.pallas import tpu as pltpu
from jax.sharding import PartitionSpec as P

LN_EPS = 1e-6
MESH = pl.DeviceIdType.MESH
TOKEN_AXES = ("batch", "time", "region")
F32, BF16 = jnp.float32, jnp.bfloat16
NT = (((1,), (1,)), ((), ()))
TN = (((0,), (0,)), ((), ()))
NN = (((1,), (0,)), ((), ()))
LOG2E = 1.4426950408889634
TERMS, WIDE = 3, 16
BIG, MID = 60_000_000, 50_000_000
LANES, TOK, ENC, DEC = 128, 256, 1280, 512
PART, HID, CODED, KEYS, ALL = 640, 2560, 640, 2048, 1536


def vm(*shape):
    return pltpu.VMEM(shape, BF16)


def vmf(*shape):
    return pltpu.VMEM(shape, F32)


def mm(lhs, rhs, dims=NN):
    return lax.dot_general(lhs, rhs, dims, preferred_element_type=F32)


def norm(x, gain, shift):
    mean = jnp.mean(x, axis=-1, keepdims=True)
    cen = x - mean
    var = jnp.mean(cen * cen, axis=-1, keepdims=True)
    return cen * lax.rsqrt(var + LN_EPS) * gain + shift


def norm_rows(src, dst, gain, shift, step):
    for i in range(src.shape[0] // step):
        rows = slice(i * step, (i + 1) * step)
        dst[rows, :] = norm(src[rows, :].astype(F32), gain, shift).astype(BF16)


def gelu(x):
    return 0.5 * x * (1.0 + lax.erf(x * (0.5 ** 0.5)))


def column(row):
    return jnp.broadcast_to(row, (LANES, row.shape[1])).T


def twice(col):
    return jnp.concatenate([col, col], axis=1)


def neighbours():
    time, region = lax.axis_index("time"), lax.axis_index("region")
    mate = {"time": time, "region": region + 1 - 2 * (region % 2)}
    across = {"time": time, "region": (region + 2) % 4}
    along = {"time": 1 - time, "region": region}
    return mate, across, along


def greet(peers):
    for peer in peers:
        pl.semaphore_signal(pltpu.get_barrier_semaphore(), inc=1, device_id=peer, device_id_type=MESH)


def greeted(peers):
    pl.semaphore_wait(pltpu.get_barrier_semaphore(), len(peers))


def push(src, dst, send, recv, peer):
    return pltpu.make_async_remote_copy(src_ref=src, dst_ref=dst, send_sem=send, recv_sem=recv, device_id=peer, device_id_type=MESH)


class Gather:
    def __init__(self, src, slots, send, recv):
        self.mate, self.across, self.along = neighbours()
        half = slots.shape[1] // 2
        top, low = pl.ds(0, half), pl.ds(half, half)
        c = lambda i, s, d, peer: push(s, d, send.at[i], recv.at[i], peer)
        self.first = [c(0, src, slots.at[1], self.mate), c(1, src, slots.at[2], self.across), c(2, src, slots.at[4], self.along)]
        self.from_x = [c(3, slots.at[2, top], slots.at[6, top], self.along), c(4, slots.at[2], slots.at[3], self.mate)]
        self.from_y = [c(5, slots.at[4, low], slots.at[6, low], self.across), c(6, slots.at[4], slots.at[5], self.mate)]
        self.last = [c(7, slots.at[6, top], slots.at[7, top], self.mate), c(8, slots.at[6, low], slots.at[7, low], self.mate)]

    def start(self):
        for copy in self.first:
            copy.start()

    def relay(self):
        self.first[1].wait_recv()
        for copy in self.from_x:
            copy.start()
        self.first[2].wait_recv()
        for copy in self.from_y:
            copy.start()

    def relay_last(self):
        self.from_x[0].wait_recv()
        self.last[0].start()
        self.from_y[0].wait_recv()
        self.last[1].start()

    def finish(self):
        for copy in (self.first[0], self.from_x[1], self.from_y[1], *self.last):
            copy.wait_recv()

    def drain(self):
        for copy in (*self.first, *self.from_x, *self.from_y, *self.last):
            copy.wait_send()


def encoder_kernel(mask, b_embed, patches_in, enc_pos_in, dec_pos, vec_in, fin_in, w_embed, w_qkv, w_o, w_one, w_two, w_dec,
                   dall,
                   zbuf, patches, enc_pos, vec, fin, wemb, wqkv, wo, w1, w2, wdec, vecs, ebuf, drecv, csum, xrecv, hb, h, a, low_a, qkv, att, peer_att, acc, g, dsrc, bcol,
                   wsem, esem, lsem, esend, erecv, xsend, xrecvs, gsend, grecv, osem):
    layers = w_qkv.shape[0]
    core = lax.axis_index("region") % 2
    mate, across, along = peers = neighbours()
    width = h.shape[1]
    heads = 8
    part = att.shape[0]
    dim = part // heads
    feats = pl.ds(pl.multiple_of(core * part, LANES), part)
    other_feats = pl.ds(pl.multiple_of((1 - core) * part, LANES), part)
    mine = pl.ds(pl.multiple_of(core * LANES, LANES), LANES)
    theirs = pl.ds(pl.multiple_of((1 - core) * LANES, LANES), LANES)
    chunks = width // TOK
    groups = [(0, 1), (2, 3), (4,)]

    spans = [slice(TOK * group[0], TOK * (group[-1] + 1)) for group in groups]
    load_patches = pltpu.make_async_copy(patches_in, patches, wsem.at[2])
    load_pos = pltpu.make_async_copy(enc_pos_in, enc_pos, wsem.at[3])
    load_embed = [pltpu.make_async_copy(w_embed.at[:, span], wemb.at[:, span], esem.at[i]) for i, span in enumerate(spans)]
    late = [pltpu.make_async_copy(vec_in, vec, wsem.at[4]), pltpu.make_async_copy(fin_in, fin, wsem.at[5]),
            pltpu.make_async_copy(dec_pos, dsrc.at[:, pl.ds(0, DEC)], wsem.at[0])]
    for load in (load_patches, load_embed[0], load_pos, *load_embed[1:], *late):
        load.start()
    greet(peers)

    mrow = mask[:].astype(F32).astype(BF16)
    tok = mrow.shape[1]
    row_id = lax.broadcasted_iota(jnp.int32, (tok, tok), 0)
    col_id = lax.broadcasted_iota(jnp.int32, (tok, tok), 1)
    upper = (row_id <= col_id).astype(F32).astype(BF16)
    lower = (row_id >= col_id).astype(F32).astype(BF16)
    same = (row_id == col_id).astype(F32).astype(BF16)
    mrows = jnp.broadcast_to(mrow, (LANES, tok))
    rank = mm(mrows, upper)
    slot = lax.broadcasted_iota(jnp.int32, (LANES, tok), 0).astype(F32) + 1.0
    sel_f = jnp.where((rank == slot) & (mrows.astype(F32) > 0.5), 1.0, 0.0)
    sel = sel_f.astype(BF16)
    valid = jnp.sum(sel_f, axis=1, keepdims=True) > 0.5
    load_patches.wait()
    picked = mm(sel, patches[:]).astype(BF16)

    def layer_loads(l):
        qkv_loads = [pltpu.make_async_copy(w_qkv.at[l, w, feats], wqkv.at[pl.ds(w * part, part)], lsem.at[l, w]) for w in range(3)]
        return qkv_loads + [
            pltpu.make_async_copy(w_o.at[l], wo, lsem.at[l, 3]),
            pltpu.make_async_copy(w_one.at[l], w1, lsem.at[l, 4]),
            pltpu.make_async_copy(w_two.at[l], w2, lsem.at[l, 5]),
        ]

    load_dec = pltpu.make_async_copy(w_dec, wdec, wsem.at[1])

    pairs, xs1, ys1, f1, f2 = [], [], [], [], []
    for j in range(chunks):
        pairs.append(push(ebuf.at[j, 1 - core], drecv.at[j], esend.at[0, j], erecv.at[0, j], mate))
        xs1.append(push(csum.at[j], xrecv.at[j], esend.at[1, j], erecv.at[1, j], across))
        ys1.append(push(hb.at[0, core, j], hb.at[1, core, j], esend.at[2, j], erecv.at[2, j], along))
        f1.append(push(hb.at[0, core, j], hb.at[0, core, j], esend.at[3, j], erecv.at[3, j], mate))
        f2.append(push(hb.at[1, core, j], hb.at[1, core, j], esend.at[4, j], erecv.at[4, j], mate))
    for n, group in enumerate(groups):
        cols = spans[n]
        load_embed[n].wait()
        if n == 0:
            load_pos.wait()
        e = mm(picked, wemb[:, cols]) + b_embed[cols].reshape(1, -1) + mm(sel, enc_pos[:, cols])
        e = jnp.where(valid, e, 0.0).astype(BF16)
        for i, j in enumerate(group):
            ebuf[j, 0] = e[:, TOK * i:TOK * i + LANES]
            ebuf[j, 1] = e[:, TOK * i + LANES:TOK * (i + 1)]
        if group[0] == 0:
            greeted(peers)
        for j in group:
            pairs[j].start()
    for load in layer_loads(0):
        load.start()
    for j in range(chunks):
        pairs[j].wait_recv()
        csum[j] = ebuf[j, core] + drecv[j]
        xs1[j].start()
    code = mm(lower, mrows, NT) * mm(same, mrows, NT)
    dsrc[:, DEC:CODED] = code.astype(BF16)
    for load in late:
        load.wait()
    vecs[layers, 0:2, :] = fin[:]
    for l in range(layers):
        vecs[l] = vec[:, l, :]
        bcol[l, 0] = column(vec[4, l:l + 1, feats])
        bcol[l, 1] = column(vec[5, l:l + 1, feats])
    for j in range(chunks):
        xs1[j].wait_recv()
        hb[0, core, j] = csum[j] + xrecv[j]
        ys1[j].start()
        f1[j].start()
    for j in range(chunks):
        ys1[j].wait_recv()
        f2[j].start()
    in_f1 = [push(hb.at[0, 1 - core, j], hb.at[0, 1 - core, j], esend.at[3, j], erecv.at[3, j], mate) for j in range(chunks)]
    in_f2 = [push(hb.at[1, 1 - core, j], hb.at[1, 1 - core, j], esend.at[4, j], erecv.at[4, j], mate) for j in range(chunks)]
    for j in range(chunks):
        in_f1[j].wait_recv()
        in_f2[j].wait_recv()
    for j in range(chunks):
        for copy in (pairs[j], xs1[j], ys1[j], f1[j], f2[j]):
            copy.wait_send()

    gather = Gather(dsrc, dall, gsend, grecv)
    own = pltpu.make_async_copy(dsrc, dall.at[0], osem.at[0])
    own.start()
    gather.start()

    for t in range(2):
        for half in range(2):
            for j in range(chunks):
                h[LANES * t:LANES * (t + 1), TOK * j + LANES * half:TOK * j + LANES * half + LANES] = hb[t, half, j]

    half_att = part // 2
    send_att = [push(att.at[pl.ds(i * half_att, half_att), theirs], peer_att.at[pl.ds(i * half_att, half_att)], xsend.at[2 + i], xrecvs.at[2 + i], mate)
                for i in range(2)]
    send_rows = push(a.at[mine], a.at[mine], xsend.at[1], xrecvs.at[1], mate)
    get_rows = push(a.at[theirs], a.at[theirs], xsend.at[1], xrecvs.at[1], mate)

    def scores(hd):
        rows = slice(hd * dim, (hd + 1) * dim)
        return mm(qkv[part + hd * dim:part + (hd + 1) * dim, :], qkv[rows, :], TN)

    def layer(l, _):
        def row(i):
            return vecs[l, i:i + 1, :]

        *qkv_loads, load_o, load_one, load_two = layer_loads(l)
        for load in qkv_loads:
            load.wait()
        mid = 3 * part // 2
        low = mm(wqkv[:mid, :], a[:], NT)
        top = mm(wqkv[mid:, :], a[:], NT)
        qkv[:part, :] = (low[:part] + twice(bcol[l, 0])).astype(BF16)
        qkv[part:mid, :] = low[part:].astype(BF16)
        qkv[mid:2 * part, :] = top[:2 * part - mid].astype(BF16)
        qkv[2 * part:, :] = (top[2 * part - mid:] + twice(bcol[l, 1])).astype(BF16)
        ahead = layer_loads(layers - 1)

        @pl.when(l == 0)
        def _():
            for load in (*ahead[:3], load_dec):
                load.start()

        scale = dim ** -0.5 * LOG2E
        s = scores(0)
        for hd in range(heads):
            nxt = scores(hd + 1) if hd + 1 < heads else None
            p = jnp.exp2(s * scale - jnp.max(s, axis=0, keepdims=True) * scale)
            total = jnp.sum(p, axis=0, keepdims=True)
            o = mm(qkv[2 * part + hd * dim:2 * part + (hd + 1) * dim, :], p.astype(BF16))
            att[hd * dim:(hd + 1) * dim, :] = (o * (1.0 / total)).astype(BF16)
            s = nxt
            if hd + 1 == heads // 2:
                send_att[0].start()
        send_att[1].start()
        load_o.wait()
        acc[:] = mm(att[:, mine], wo[feats, :], TN)
        for copy in send_att:
            copy.wait_recv()
        r = acc[:] + mm(peer_att[:], wo[other_feats, :], TN)
        rows = (h[mine, :].astype(F32) + r + row(6)).astype(BF16)
        h[mine, :] = rows
        low_a[:] = norm(rows.astype(F32), row(2), row(3)).astype(BF16)
        for copy in send_att:
            copy.wait_send()
        pl.when(l == 0)(ahead[3].start)
        load_one.wait()
        for j in range(g.shape[1] // TOK):
            cols = slice(TOK * j, TOK * (j + 1))
            at = (TOK * j) % width
            bias = row(8 + (TOK * j) // width)[:, at:at + TOK]
            g[:, cols] = gelu(mm(low_a[:], w1[:, cols]) + bias).astype(BF16)
        pl.when(l == 0)(ahead[4].start)
        pl.when(l > 0)(gather.relay_last)
        load_two.wait()
        rows = (h[mine, :].astype(F32) + mm(g[:], w2[:]) + row(7)).astype(BF16)
        h[mine, :] = rows
        pl.when(l == 0)(ahead[5].start)
        a[mine, :] = norm(rows.astype(F32), vecs[l + 1, 0:1, :], vecs[l + 1, 1:2, :]).astype(BF16)
        send_rows.start()
        pl.when(l == 0)(gather.relay)
        get_rows.wait_recv()
        send_rows.wait_send()
        return 0

    norm_rows(h, a, vecs[0, 0:1, :], vecs[0, 1:2, :], 64)
    lax.fori_loop(0, layers, layer, 0)
    load_dec.wait()
    zbuf[:] = mm(a[:], wdec[:]).astype(BF16)
    z_copy = pltpu.make_async_copy(zbuf, dall.at[8, :, pl.ds(0, DEC)], osem.at[1])
    z_copy.start()
    gather.finish()
    gather.drain()
    own.wait()
    z_copy.wait()


def attend(q, kt, vt, att, buf, peak, state, dim, tiles, first, last, between=None):
    deep = TERMS * dim
    tops, sums, outs = state
    crew = max(1, WIDE // len(tiles))
    units = att.shape[0] // dim // crew

    def rows_of(hd, size):
        start = hd * size
        return pl.ds(start if isinstance(start, int) else pl.multiple_of(start, size), size)

    def begin(hd, spot):
        top = jnp.max(peak[spot], axis=0, keepdims=True)
        if first:
            return top, jnp.zeros((8, TOK), F32), jnp.zeros((dim, TOK), F32)
        old = tops[hd]
        top = jnp.maximum(old[0:1], top)
        fade = jnp.exp2(old[0:1] - top)
        return top, sums[hd] * fade, outs[rows_of(hd, dim), :] * fade

    def end(hd, top, total, out):
        if last:
            total = jnp.sum(total, axis=0, keepdims=True)
            att[rows_of(hd, dim), :] = (out * (1.0 / total)).astype(BF16)
        else:
            tops[hd] = jnp.broadcast_to(top, (8, TOK))
            sums[hd] = total
            outs[rows_of(hd, dim), :] = out

    def step(score_unit, score_slot, unit, slot):
        best = [jnp.full((8, TOK), -jnp.inf, F32)] * crew
        if unit is not None:
            runs = [begin(unit * crew + n, slot * crew + n) for n in range(crew)]
        for n in range(crew):
            for i, tile in enumerate(tiles):
                keys = slice(TOK * (n * len(tiles) + i), TOK * (n * len(tiles) + i + 1))
                cols = slice(TOK * tile, TOK * (tile + 1))
                if score_unit is not None:
                    rows = rows_of(score_unit * crew + n, deep)
                    s = mm(kt[rows, cols], q[rows, :], TN)
                    buf[score_slot][keys, :] = s
                    best[n] = jnp.maximum(best[n], jnp.max(s.reshape(-1, 8, TOK), axis=0))
                if unit is not None:
                    top, total, out = runs[n]
                    p = jnp.exp2(buf[slot][keys, :] - top)
                    total = total + jnp.sum(p.reshape(-1, 8, TOK), axis=0)
                    out = out + mm(vt[rows_of(unit * crew + n, dim), cols], p.astype(BF16))
                    runs[n] = top, total, out
        for n in range(crew):
            if score_unit is not None:
                peak[score_slot * crew + n] = best[n]
            if unit is not None:
                end(unit * crew + n, *runs[n])

    def body(i, _):
        step(2 * i + 1, 1, 2 * i, 0)
        step(2 * i + 2, 0, 2 * i + 1, 1)
        return 0

    step(0, 0, None, None)
    half = units // 4
    lax.fori_loop(0, half, body, 0)
    if between:
        between()
    lax.fori_loop(half, units // 2 - 1, body, 0)
    step(units - 1, 1, units - 2, 0)
    step(None, None, units - 1, 1)


def block_tail(h, att, a, g, vec, l, wo, w1, w2, rows):
    h[rows, :] = (h[rows, :].astype(F32) + mm(att[:, rows], wo[l], TN) + vec[6, l:l + 1, :]).astype(BF16)
    a[rows, :] = norm(h[rows, :].astype(F32), vec[2, l:l + 1, :], vec[3, l:l + 1, :]).astype(BF16)
    width = h.shape[1]
    for j in range(w1.shape[2] // width):
        cols = slice(width * j, width * (j + 1))
        g[rows, cols] = gelu(mm(a[rows, :], w1[l, :, cols]) + vec[8 + j, l:l + 1, :]).astype(BF16)
    h[rows, :] = (h[rows, :].astype(F32) + mm(g[rows, :], w2[l]) + vec[7, l:l + 1, :]).astype(BF16)


class Halves:
    def __init__(self, src, tiles, send, recv):
        self.mate, self.across, self.along = neighbours()
        half = tiles.shape[1] // 2
        top, low = pl.ds(0, half), pl.ds(half, half)
        made = []

        def c(s, d, peer):
            made.append(push(s, d, send.at[len(made)], recv.at[len(made)], peer))
            return made[-1]

        self.own = [[c(src.at[r], tiles.at[2 + 2 * n, top], self.across), c(src.at[r], tiles.at[2 + 2 * n, low], self.along),
                     c(src.at[r], tiles.at[1, r], self.mate)] for n, r in enumerate((top, low))]
        self.mates = [[c(tiles.at[2 + 2 * n, r], tiles.at[3 + 2 * n, r], self.mate) for r in (top, low)] for n in range(3)]
        self.corner = [c(tiles.at[2, top], tiles.at[6, top], self.along), c(tiles.at[4, low], tiles.at[6, low], self.across)]
        self.made = made

    def start(self, n):
        for copy in self.own[n]:
            copy.start()

    def relay(self, n):
        for i in range(2):
            self.own[n][i].wait_recv()
        self.corner[n].start()
        for copy in self.mates[n]:
            copy.start()

    def relay_corner(self):
        for n in range(2):
            self.corner[n].wait_recv()
            self.mates[2][n].start()

    def from_mate(self, n):
        for copy in self.mates[n]:
            copy.wait_recv()

    def drain(self):
        for copy in self.made:
            copy.wait_send()


def decoder_kernel(token, vec, fin, dall, w_qkv, w_o, w_one, w_two, y_out,
                   wqkv, wo, w1, w2, z, dslots, h, a, own, aall, arecv, kt, vt, q, att, g, buf0, buf1, peak, tops, sums, outs, bcol,
                   wsem, dsem, gsend, grecv):
    width = h.shape[1]
    layers = wqkv.shape[0]
    slots = dslots.shape[0]
    peers = neighbours()
    greet(peers)
    blocks = [pltpu.make_async_copy(dall.at[i], dslots.at[i], dsem.at[i]) for i in range(slots)]
    pairs = ((w_qkv, wqkv), (w_o, wo), (w_one, w1), (w_two, w2))
    loads = [[pltpu.make_async_copy(src.at[l], dst.at[l], wsem.at[l, i]) for i, (src, dst) in enumerate(pairs)] for l in range(layers)]
    blocks.append(pltpu.make_async_copy(dall.at[slots, :, pl.ds(0, DEC)], z, dsem.at[slots]))
    loads[0][0].start()
    for block in reversed(blocks):
        block.start()

    for l in range(layers):
        bcol[l, 0] = column(vec[4, l:l + 1, :])
        bcol[l, 1] = column(vec[5, l:l + 1, :])
    lane = lax.broadcasted_iota(jnp.int32, (TOK, LANES), 1).astype(F32) + 1.0
    buf, state = (buf0, buf1), (tops, sums, outs)

    dim = width // 16

    def queries(l, rows):
        rest = (mm(wqkv[l, 0:width, :], rows, NT) + twice(bcol[l, 0])).astype(BF16).astype(F32) * (dim ** -0.5 * LOG2E)
        for t in range(TERMS):
            term = rest.astype(BF16)
            rest = rest - term.astype(F32)
            for hd in range(width // dim):
                q[(TERMS * hd + t) * dim:(TERMS * hd + t + 1) * dim, :] = term[hd * dim:(hd + 1) * dim]

    def keys_values(l, i):
        cols = slice(TOK * i, TOK * (i + 1))
        rows = aall[i] if l == 0 else arecv[i]
        key = mm(wqkv[l, width:2 * width, :], rows, NT).astype(BF16)
        for hd in range(width // dim):
            for t in range(TERMS):
                kt[(TERMS * hd + t) * dim:(TERMS * hd + t + 1) * dim, cols] = key[hd * dim:(hd + 1) * dim]
        vt[:, cols] = (mm(wqkv[l, 2 * width:, :], rows, NT) + twice(bcol[l, 1])).astype(BF16)

    def rows_in(i):
        code = dslots[i, :, DEC:CODED].astype(F32)
        pick = jnp.where(code == lane, 1.0, 0.0).astype(BF16)
        block = 0 if i < slots // 2 else LANES
        placed = mm(pick, z[block:block + LANES, :])
        seen = code[:, 0:1] > 0.5
        u = (jnp.where(seen, placed, token[:].astype(F32).reshape(1, -1)) + dslots[i, :, 0:DEC].astype(F32)).astype(BF16)
        if i == 0:
            h[:] = u
        aall[i] = norm(u.astype(F32), vec[0, 0:1, :], vec[1, 0:1, :]).astype(BF16)

    for block in blocks:
        block.wait()
    loads[0][0].wait()
    for load in loads[0][1:] + loads[1]:
        load.start()
    rows_in(0)
    queries(0, aall[0])
    for i in range(1, slots):
        rows_in(i)
    for i in range(slots):
        keys_values(0, i)
    attend(q, kt, vt, att, buf, peak, state, dim, range(slots), True, True)
    for load in loads[0][1:]:
        load.wait()
    gather = Halves(own, arecv, gsend, grecv)
    ways = (slice(0, LANES), slice(LANES, TOK))
    for n, rows in enumerate(ways):
        block_tail(h, att, a, g, vec, 0, wo, w1, w2, rows)
        own[rows, :] = norm(h[rows, :].astype(F32), vec[0, 1:2, :], vec[1, 1:2, :]).astype(BF16)
        if n == 0:
            greeted(peers)
        gather.start(n)
    arecv[0] = own[:]
    loads[1][0].wait()
    queries(1, own[:])
    keys_values(1, 0)
    for n in range(2):
        gather.own[n][2].wait_recv()
    keys_values(1, 1)
    attend(q, kt, vt, att, buf, peak, state, dim, (0, 1), True, False)
    for n in range(2):
        gather.relay(n)
        keys_values(1, 2 + 2 * n)
        gather.from_mate(n)
        keys_values(1, 3 + 2 * n)
        attend(q, kt, vt, att, buf, peak, state, dim, (2 + 2 * n, 3 + 2 * n), False, False)
    gather.relay_corner()
    keys_values(1, 6)
    gather.from_mate(2)
    keys_values(1, 7)
    attend(q, kt, vt, att, buf, peak, state, dim, (6, 7), False, True)
    for load in loads[1][1:]:
        load.wait()
    block_tail(h, att, a, g, vec, 1, wo, w1, w2, slice(0, TOK))
    norm_rows(h, y_out, fin[0:1, :], fin[1:2, :], LANES)
    gather.drain()


VM = pl.BlockSpec(memory_space=pltpu.VMEM)
HB = pl.BlockSpec(memory_space=pl.ANY)


def solution(mesh):
    def local_step(patches, enc_pos, vis_mask, dec_pos, w_embed, b_embed, enc_vec, enc_wqkv, enc_wo, enc_w1, enc_w2, enc_final, w_dec_in, mask_token, dec_vec, dec_wqkv, dec_wo, dec_w1, dec_w2, dec_final, w_out):
        layers = enc_vec.shape[0]
        evec = jnp.transpose(enc_vec, (1, 0, 2))
        dvec = jnp.transpose(dec_vec, (1, 0, 2))
        ewqkv = jnp.transpose(enc_wqkv, (0, 2, 3, 4, 1)).reshape(layers, 3, ENC, ENC)
        ewo = enc_wo.reshape(layers, ENC, ENC)
        dwqkv = jnp.transpose(dec_wqkv, (0, 2, 3, 4, 1)).reshape(layers, ALL, DEC)
        dwo = dec_wo.reshape(layers, DEC, DEC)
        dma = pltpu.SemaphoreType.DMA
        chunks = ENC // TOK
        piece = (chunks, LANES, LANES)
        dall = pl.pallas_call(
            encoder_kernel,
            out_shape=jax.ShapeDtypeStruct((LANES, TOK, CODED), BF16),
            in_specs=[VM] * 2 + [HB] * 11,
            out_specs=HB,
            scratch_shapes=[
                vm(TOK, DEC), vm(TOK, ALL), vm(TOK, ENC), vmf(12, layers, ENC), vmf(2, ENC), vm(ALL, ENC),
                vm(3 * PART, ENC), vm(ENC, ENC), vm(ENC, 2 * HID), vm(2 * HID, ENC), vm(ENC, DEC), vmf(layers + 1, 12, ENC),
                vm(chunks, 2, LANES, LANES), vm(*piece), vm(*piece), vm(*piece), vm(2, 2, *piece),
                vm(TOK, ENC), vm(TOK, ENC), vm(LANES, ENC), vm(3 * PART, TOK), vm(PART, TOK), vm(PART, LANES), vmf(LANES, ENC), vm(LANES, 2 * HID),
                vm(TOK, CODED), vmf(layers, 2, PART, LANES),
                dma((6,)), dma((chunks,)), dma((layers, 6)), dma((chunks, chunks)), dma((chunks, chunks)), dma((4,)), dma((4,)), dma((9,)), dma((9,)), dma((2,)),
            ],
            compiler_params=pltpu.CompilerParams(collective_id=0, has_side_effects=True, vmem_limit_bytes=BIG),
            name="encoder",
        )(vis_mask.reshape(1, -1), b_embed, patches, enc_pos, dec_pos, evec, enc_final, w_embed, ewqkv, ewo, enc_w1, enc_w2, w_dec_in)
        y = pl.pallas_call(
            decoder_kernel,
            out_shape=jax.ShapeDtypeStruct((TOK, DEC), BF16),
            in_specs=[VM] * 3 + [HB] * 5,
            out_specs=VM,
            scratch_shapes=[
                vm(layers, ALL, DEC), vm(layers, DEC, DEC), vm(layers, DEC, KEYS), vm(layers, KEYS, DEC),
                vm(TOK, DEC), vm(8, TOK, CODED), vm(TOK, DEC), vm(TOK, DEC), vm(TOK, DEC), vm(8, TOK, DEC), vm(8, TOK, DEC),
                vm(TERMS * DEC, KEYS), vm(DEC, KEYS), vm(TERMS * DEC, TOK), vm(DEC, TOK), vm(TOK, KEYS),
                vmf(WIDE * TOK, TOK), vmf(WIDE * TOK, TOK), vmf(WIDE, 8, TOK), vmf(16, 8, TOK), vmf(16, 8, TOK), vmf(DEC, TOK), vmf(layers, 2, DEC, LANES),
                dma((layers, 4)), dma((9,)), dma((14,)), dma((14,)),
            ],
            compiler_params=pltpu.CompilerParams(collective_id=1, has_side_effects=True, vmem_limit_bytes=MID),
            name="decoder",
        )(mask_token, dvec, dec_final, dall, dwqkv, dwo, dec_w1, dec_w2)
        return jnp.dot(y, w_out, preferred_element_type=F32)

    token_rows = P(TOKEN_AXES, None)
    in_specs = (token_rows, token_rows, P(TOKEN_AXES), token_rows) + (P(),) * 17
    return jax.shard_map(local_step, mesh=mesh, in_specs=in_specs, out_specs=token_rows, check_vma=False)
```

```python
import functools
import math

import jax
import jax.numpy as jnp
from jax import lax
from jax.experimental import pallas as pl
from jax.experimental.pallas import tpu as pltpu
from jax.sharding import PartitionSpec as P

LN_EPS = 1e-6
MESH = pl.DeviceIdType.MESH
TOKEN_AXES = ("batch", "time", "region")
F32, BF16 = jnp.float32, jnp.bfloat16
NT = (((1,), (1,)), ((), ()))
TN = (((0,), (0,)), ((), ()))
NN = (((1,), (0,)), ((), ()))
LOG2E = 1.4426950408889634
GROUP = 2
TERMS, WIDE = 3, 16
BIG, MID = 60_000_000, 50_000_000
LANES, TOK, ENC, DEC = 128, 256, 1280, 512
PART, HID, CODED, KEYS, ALL = 640, 2560, 640, 2048, 1536


def vm(*shape):
    return pltpu.VMEM(shape, BF16)


def vmf(*shape):
    return pltpu.VMEM(shape, F32)


def mm(lhs, rhs, dims=NN):
    return lax.dot_general(lhs, rhs, dims, preferred_element_type=F32)


def norm(x, gain, shift):
    mean = jnp.mean(x, axis=-1, keepdims=True)
    cen = x - mean
    var = jnp.mean(cen * cen, axis=-1, keepdims=True)
    return cen * lax.rsqrt(var + LN_EPS) * gain + shift


def norm_rows(src, dst, gain, shift, step):
    for i in range(src.shape[0] // step):
        rows = slice(i * step, (i + 1) * step)
        dst[rows, :] = norm(src[rows, :].astype(F32), gain, shift).astype(BF16)


def gelu(x):
    return 0.5 * x * (1.0 + lax.erf(x * (0.5 ** 0.5)))


def column(row):
    return jnp.broadcast_to(row, (LANES, row.shape[1])).T


def twice(col):
    return jnp.concatenate([col, col], axis=1)


def neighbours():
    time, region = lax.axis_index("time"), lax.axis_index("region")
    mate = {"time": time, "region": region + 1 - 2 * (region % 2)}
    across = {"time": time, "region": (region + 2) % 4}
    along = {"time": 1 - time, "region": region}
    return mate, across, along


def greet(peers):
    for peer in peers:
        pl.semaphore_signal(pltpu.get_barrier_semaphore(), inc=1, device_id=peer, device_id_type=MESH)


def greeted(peers):
    pl.semaphore_wait(pltpu.get_barrier_semaphore(), len(peers))


def push(src, dst, send, recv, peer):
    return pltpu.make_async_remote_copy(src_ref=src, dst_ref=dst, send_sem=send, recv_sem=recv, device_id=peer, device_id_type=MESH)


class Gather:
    def __init__(self, src, slots, send, recv):
        self.mate, self.across, self.along = neighbours()
        half = slots.shape[1] // 2
        top, low = pl.ds(0, half), pl.ds(half, half)
        c = lambda i, s, d, peer: push(s, d, send.at[i], recv.at[i], peer)
        self.first = [c(0, src, slots.at[1], self.mate), c(1, src, slots.at[2], self.across), c(2, src, slots.at[4], self.along)]
        self.from_x = [c(3, slots.at[2, top], slots.at[6, top], self.along), c(4, slots.at[2], slots.at[3], self.mate)]
        self.from_y = [c(5, slots.at[4, low], slots.at[6, low], self.across), c(6, slots.at[4], slots.at[5], self.mate)]
        self.last = [c(7, slots.at[6, top], slots.at[7, top], self.mate), c(8, slots.at[6, low], slots.at[7, low], self.mate)]

    def start(self):
        for copy in self.first:
            copy.start()

    def relay(self):
        self.first[1].wait_recv()
        for copy in self.from_x:
            copy.start()
        self.first[2].wait_recv()
        for copy in self.from_y:
            copy.start()

    def relay_last(self):
        self.from_x[0].wait_recv()
        self.last[0].start()
        self.from_y[0].wait_recv()
        self.last[1].start()

    def finish(self):
        for copy in (self.first[0], self.from_x[1], self.from_y[1], *self.last):
            copy.wait_recv()

    def drain(self):
        for copy in (*self.first, *self.from_x, *self.from_y, *self.last):
            copy.wait_send()


def encoder_kernel(mask, b_embed, patches_in, enc_pos_in, dec_pos, vec_in, fin_in, w_embed, w_qkv, w_o, w_one, w_two, w_dec,
                   dall,
                   zbuf, patches, enc_pos, vec, fin, wemb, wqkv, wo, w1, w2, wdec, vecs, ebuf, drecv, csum, xrecv, hb, h, a, low_a, qkv, att, peer_att, acc, g, dsrc, bcol,
                   wsem, esem, lsem, esend, erecv, xsend, xrecvs, gsend, grecv, osem):
    layers = w_qkv.shape[0]
    core = lax.axis_index("region") % 2
    mate, across, along = peers = neighbours()
    width = h.shape[1]
    heads = 8
    part = att.shape[0]
    dim = part // heads
    feats = pl.ds(pl.multiple_of(core * part, LANES), part)
    other_feats = pl.ds(pl.multiple_of((1 - core) * part, LANES), part)
    mine = pl.ds(pl.multiple_of(core * LANES, LANES), LANES)
    theirs = pl.ds(pl.multiple_of((1 - core) * LANES, LANES), LANES)
    chunks = width // TOK
    groups = [(0, 1), (2, 3), (4,)]

    spans = [slice(TOK * group[0], TOK * (group[-1] + 1)) for group in groups]
    load_patches = pltpu.make_async_copy(patches_in, patches, wsem.at[2])
    load_pos = pltpu.make_async_copy(enc_pos_in, enc_pos, wsem.at[3])
    load_embed = [pltpu.make_async_copy(w_embed.at[:, span], wemb.at[:, span], esem.at[i]) for i, span in enumerate(spans)]
    late = [pltpu.make_async_copy(vec_in, vec, wsem.at[4]), pltpu.make_async_copy(fin_in, fin, wsem.at[5]),
            pltpu.make_async_copy(dec_pos, dsrc.at[:, pl.ds(0, DEC)], wsem.at[0])]
    for load in (load_patches, load_embed[0], load_pos, *load_embed[1:], *late):
        load.start()
    greet(peers)

    mrow = mask[:].astype(F32).astype(BF16)
    tok = mrow.shape[1]
    row_id = lax.broadcasted_iota(jnp.int32, (tok, tok), 0)
    col_id = lax.broadcasted_iota(jnp.int32, (tok, tok), 1)
    upper = (row_id <= col_id).astype(F32).astype(BF16)
    lower = (row_id >= col_id).astype(F32).astype(BF16)
    same = (row_id == col_id).astype(F32).astype(BF16)
    mrows = jnp.broadcast_to(mrow, (LANES, tok))
    rank = mm(mrows, upper)
    slot = lax.broadcasted_iota(jnp.int32, (LANES, tok), 0).astype(F32) + 1.0
    sel_f = jnp.where((rank == slot) & (mrows.astype(F32) > 0.5), 1.0, 0.0)
    sel = sel_f.astype(BF16)
    valid = jnp.sum(sel_f, axis=1, keepdims=True) > 0.5
    load_patches.wait()
    picked = mm(sel, patches[:]).astype(BF16)

    def layer_loads(l):
        qkv_loads = [pltpu.make_async_copy(w_qkv.at[l, w, feats], wqkv.at[pl.ds(w * part, part)], lsem.at[l, w]) for w in range(3)]
        return qkv_loads + [
            pltpu.make_async_copy(w_o.at[l], wo, lsem.at[l, 3]),
            pltpu.make_async_copy(w_one.at[l], w1, lsem.at[l, 4]),
            pltpu.make_async_copy(w_two.at[l], w2, lsem.at[l, 5]),
        ]

    load_dec = pltpu.make_async_copy(w_dec, wdec, wsem.at[1])

    pairs, xs1, ys1, f1, f2 = [], [], [], [], []
    for j in range(chunks):
        pairs.append(push(ebuf.at[j, 1 - core], drecv.at[j], esend.at[0, j], erecv.at[0, j], mate))
        xs1.append(push(csum.at[j], xrecv.at[j], esend.at[1, j], erecv.at[1, j], across))
        ys1.append(push(hb.at[0, core, j], hb.at[1, core, j], esend.at[2, j], erecv.at[2, j], along))
        f1.append(push(hb.at[0, core, j], hb.at[0, core, j], esend.at[3, j], erecv.at[3, j], mate))
        f2.append(push(hb.at[1, core, j], hb.at[1, core, j], esend.at[4, j], erecv.at[4, j], mate))
    for n, group in enumerate(groups):
        cols = spans[n]
        load_embed[n].wait()
        if n == 0:
            load_pos.wait()
        e = mm(picked, wemb[:, cols]) + b_embed[cols].reshape(1, -1) + mm(sel, enc_pos[:, cols])
        e = jnp.where(valid, e, 0.0).astype(BF16)
        for i, j in enumerate(group):
            ebuf[j, 0] = e[:, TOK * i:TOK * i + LANES]
            ebuf[j, 1] = e[:, TOK * i + LANES:TOK * (i + 1)]
        if group[0] == 0:
            greeted(peers)
        for j in group:
            pairs[j].start()
    for load in layer_loads(0):
        load.start()
    for j in range(chunks):
        pairs[j].wait_recv()
        csum[j] = ebuf[j, core] + drecv[j]
        xs1[j].start()
    code = mm(lower, mrows, NT) * mm(same, mrows, NT)
    dsrc[:, DEC:CODED] = code.astype(BF16)
    for load in late:
        load.wait()
    vecs[layers, 0:2, :] = fin[:]
    for l in range(layers):
        vecs[l] = vec[:, l, :]
        bcol[l, 0] = column(vec[4, l:l + 1, feats])
        bcol[l, 1] = column(vec[5, l:l + 1, feats])
    for j in range(chunks):
        xs1[j].wait_recv()
        hb[0, core, j] = csum[j] + xrecv[j]
        ys1[j].start()
        f1[j].start()
    for j in range(chunks):
        ys1[j].wait_recv()
        f2[j].start()
    in_f1 = [push(hb.at[0, 1 - core, j], hb.at[0, 1 - core, j], esend.at[3, j], erecv.at[3, j], mate) for j in range(chunks)]
    in_f2 = [push(hb.at[1, 1 - core, j], hb.at[1, 1 - core, j], esend.at[4, j], erecv.at[4, j], mate) for j in range(chunks)]
    for j in range(chunks):
        in_f1[j].wait_recv()
        in_f2[j].wait_recv()
    for j in range(chunks):
        for copy in (pairs[j], xs1[j], ys1[j], f1[j], f2[j]):
            copy.wait_send()

    gather = Gather(dsrc, dall, gsend, grecv)
    own = pltpu.make_async_copy(dsrc, dall.at[0], osem.at[0])
    own.start()
    gather.start()

    for t in range(2):
        for half in range(2):
            for j in range(chunks):
                h[LANES * t:LANES * (t + 1), TOK * j + LANES * half:TOK * j + LANES * half + LANES] = hb[t, half, j]

    half_att = part // 2
    send_att = [push(att.at[pl.ds(i * half_att, half_att), theirs], peer_att.at[pl.ds(i * half_att, half_att)], xsend.at[2 + i], xrecvs.at[2 + i], mate)
                for i in range(2)]
    send_rows = push(a.at[mine], a.at[mine], xsend.at[1], xrecvs.at[1], mate)
    get_rows = push(a.at[theirs], a.at[theirs], xsend.at[1], xrecvs.at[1], mate)

    def scores(hd):
        rows = slice(hd * dim, (hd + 1) * dim)
        return mm(qkv[part + hd * dim:part + (hd + 1) * dim, :], qkv[rows, :], TN)

    def layer(l, _):
        def row(i):
            return vecs[l, i:i + 1, :]

        *qkv_loads, load_o, load_one, load_two = layer_loads(l)
        for load in qkv_loads:
            load.wait()
        mid = 3 * part // 2
        low = mm(wqkv[:mid, :], a[:], NT)
        top = mm(wqkv[mid:, :], a[:], NT)
        qkv[:part, :] = (low[:part] + twice(bcol[l, 0])).astype(BF16)
        qkv[part:mid, :] = low[part:].astype(BF16)
        qkv[mid:2 * part, :] = top[:2 * part - mid].astype(BF16)
        qkv[2 * part:, :] = (top[2 * part - mid:] + twice(bcol[l, 1])).astype(BF16)
        ahead = layer_loads(layers - 1)

        @pl.when(l == 0)
        def _():
            for load in (*ahead[:3], load_dec):
                load.start()

        scale = dim ** -0.5 * LOG2E
        s = scores(0)
        for hd in range(heads):
            nxt = scores(hd + 1) if hd + 1 < heads else None
            p = jnp.exp2(s * scale - jnp.max(s, axis=0, keepdims=True) * scale)
            total = jnp.sum(p, axis=0, keepdims=True)
            o = mm(qkv[2 * part + hd * dim:2 * part + (hd + 1) * dim, :], p.astype(BF16))
            att[hd * dim:(hd + 1) * dim, :] = (o * (1.0 / total)).astype(BF16)
            s = nxt
            if hd + 1 == heads // 2:
                send_att[0].start()
        send_att[1].start()
        load_o.wait()
        acc[:] = mm(att[:, mine], wo[feats, :], TN)
        for copy in send_att:
            copy.wait_recv()
        r = acc[:] + mm(peer_att[:], wo[other_feats, :], TN)
        rows = (h[mine, :].astype(F32) + r + row(6)).astype(BF16)
        h[mine, :] = rows
        low_a[:] = norm(rows.astype(F32), row(2), row(3)).astype(BF16)
        for copy in send_att:
            copy.wait_send()
        pl.when(l == 0)(ahead[3].start)
        load_one.wait()
        for j in range(g.shape[1] // TOK):
            cols = slice(TOK * j, TOK * (j + 1))
            at = (TOK * j) % width
            bias = row(8 + (TOK * j) // width)[:, at:at + TOK]
            g[:, cols] = gelu(mm(low_a[:], w1[:, cols]) + bias).astype(BF16)
        pl.when(l == 0)(ahead[4].start)
        pl.when(l > 0)(gather.relay_last)
        load_two.wait()
        rows = (h[mine, :].astype(F32) + mm(g[:], w2[:]) + row(7)).astype(BF16)
        h[mine, :] = rows
        pl.when(l == 0)(ahead[5].start)
        a[mine, :] = norm(rows.astype(F32), vecs[l + 1, 0:1, :], vecs[l + 1, 1:2, :]).astype(BF16)
        send_rows.start()
        pl.when(l == 0)(gather.relay)
        get_rows.wait_recv()
        send_rows.wait_send()
        return 0

    norm_rows(h, a, vecs[0, 0:1, :], vecs[0, 1:2, :], 64)
    lax.fori_loop(0, layers, layer, 0)
    load_dec.wait()
    zbuf[:] = mm(a[:], wdec[:]).astype(BF16)
    z_copy = pltpu.make_async_copy(zbuf, dall.at[8, :, pl.ds(0, DEC)], osem.at[1])
    z_copy.start()
    gather.finish()
    gather.drain()
    own.wait()
    z_copy.wait()


def attend(q, kt, vt, att, buf, peak, state, dim, tiles, first, last, between=None):
    deep = TERMS * dim
    tops, sums, outs = state
    crew = max(1, WIDE // len(tiles))
    units = att.shape[0] // dim // crew

    def rows_of(hd, size):
        start = hd * size
        return pl.ds(start if isinstance(start, int) else pl.multiple_of(start, size), size)

    def begin(hd, spot):
        top = jnp.max(peak[spot], axis=0, keepdims=True)
        if first:
            return top, jnp.zeros((8, TOK), F32), jnp.zeros((dim, TOK), F32)
        old = tops[hd]
        top = jnp.maximum(old[0:1], top)
        fade = jnp.exp2(old[0:1] - top)
        return top, sums[hd] * fade, outs[rows_of(hd, dim), :] * fade

    def end(hd, top, total, out):
        if last:
            total = jnp.sum(total, axis=0, keepdims=True)
            att[rows_of(hd, dim), :] = (out * (1.0 / total)).astype(BF16)
        else:
            tops[hd] = jnp.broadcast_to(top, (8, TOK))
            sums[hd] = total
            outs[rows_of(hd, dim), :] = out

    def step(score_unit, score_slot, unit, slot):
        best = [jnp.full((8, TOK), -jnp.inf, F32)] * crew
        if unit is not None:
            runs = [begin(unit * crew + n, slot * crew + n) for n in range(crew)]
        for n in range(crew):
            for i, tile in enumerate(tiles):
                keys = slice(TOK * (n * len(tiles) + i), TOK * (n * len(tiles) + i + 1))
                cols = slice(TOK * tile, TOK * (tile + 1))
                if score_unit is not None:
                    rows = rows_of(score_unit * crew + n, deep)
                    s = mm(kt[rows, cols], q[rows, :], TN)
                    buf[score_slot][keys, :] = s
                    best[n] = jnp.maximum(best[n], jnp.max(s.reshape(-1, 8, TOK), axis=0))
                if unit is not None:
                    top, total, out = runs[n]
                    p = jnp.exp2(buf[slot][keys, :] - top)
                    total = total + jnp.sum(p.reshape(-1, 8, TOK), axis=0)
                    out = out + mm(vt[rows_of(unit * crew + n, dim), cols], p.astype(BF16))
                    runs[n] = top, total, out
        for n in range(crew):
            if score_unit is not None:
                peak[score_slot * crew + n] = best[n]
            if unit is not None:
                end(unit * crew + n, *runs[n])

    def body(i, _):
        step(2 * i + 1, 1, 2 * i, 0)
        step(2 * i + 2, 0, 2 * i + 1, 1)
        return 0

    step(0, 0, None, None)
    half = units // 4
    lax.fori_loop(0, half, body, 0)
    if between:
        between()
    lax.fori_loop(half, units // 2 - 1, body, 0)
    step(units - 1, 1, units - 2, 0)
    step(None, None, units - 1, 1)


def block_tail(h, att, a, g, vec, l, wo, w1, w2, rows):
    h[rows, :] = (h[rows, :].astype(F32) + mm(att[:, rows], wo[l], TN) + vec[6, l:l + 1, :]).astype(BF16)
    a[rows, :] = norm(h[rows, :].astype(F32), vec[2, l:l + 1, :], vec[3, l:l + 1, :]).astype(BF16)
    width = h.shape[1]
    for j in range(w1.shape[2] // width):
        cols = slice(width * j, width * (j + 1))
        g[rows, cols] = gelu(mm(a[rows, :], w1[l, :, cols]) + vec[8 + j, l:l + 1, :]).astype(BF16)
    h[rows, :] = (h[rows, :].astype(F32) + mm(g[rows, :], w2[l]) + vec[7, l:l + 1, :]).astype(BF16)


class Halves:
    def __init__(self, src, tiles, send, recv):
        self.mate, self.across, self.along = neighbours()
        half = tiles.shape[1] // 2
        top, low = pl.ds(0, half), pl.ds(half, half)
        made = []

        def c(s, d, peer):
            made.append(push(s, d, send.at[len(made)], recv.at[len(made)], peer))
            return made[-1]

        self.own = [[c(src.at[r], tiles.at[2 + 2 * n, top], self.across), c(src.at[r], tiles.at[2 + 2 * n, low], self.along),
                     c(src.at[r], tiles.at[1, r], self.mate)] for n, r in enumerate((top, low))]
        self.mates = [[c(tiles.at[2 + 2 * n, r], tiles.at[3 + 2 * n, r], self.mate) for r in (top, low)] for n in range(3)]
        self.corner = [c(tiles.at[2, top], tiles.at[6, top], self.along), c(tiles.at[4, low], tiles.at[6, low], self.across)]
        self.made = made

    def start(self, n):
        for copy in self.own[n]:
            copy.start()

    def relay(self, n):
        for i in range(2):
            self.own[n][i].wait_recv()
        self.corner[n].start()
        for copy in self.mates[n]:
            copy.start()

    def relay_corner(self):
        for n in range(2):
            self.corner[n].wait_recv()
            self.mates[2][n].start()

    def from_mate(self, n):
        for copy in self.mates[n]:
            copy.wait_recv()

    def drain(self):
        for copy in self.made:
            copy.wait_send()


def decoder_kernel(token, vec, fin, dall, w_qkv, w_o, w_one, w_two, y_out,
                   wqkv, wo, w1, w2, z, dslots, h, a, own, aall, arecv, kt, vt, q, att, g, buf0, buf1, peak, tops, sums, outs, bcol,
                   wsem, dsem, gsend, grecv):
    width = h.shape[1]
    layers = wqkv.shape[0]
    slots = dslots.shape[0]
    peers = neighbours()
    greet(peers)
    blocks = [pltpu.make_async_copy(dall.at[i], dslots.at[i], dsem.at[i]) for i in range(slots)]
    pairs = ((w_qkv, wqkv), (w_o, wo), (w_one, w1), (w_two, w2))
    loads = [[pltpu.make_async_copy(src.at[l], dst.at[l], wsem.at[l, i]) for i, (src, dst) in enumerate(pairs)] for l in range(layers)]
    blocks.append(pltpu.make_async_copy(dall.at[slots, :, pl.ds(0, DEC)], z, dsem.at[slots]))
    loads[0][0].start()
    for block in reversed(blocks):
        block.start()

    for l in range(layers):
        bcol[l, 0] = column(vec[4, l:l + 1, :])
        bcol[l, 1] = column(vec[5, l:l + 1, :])
    lane = lax.broadcasted_iota(jnp.int32, (GROUP * TOK, LANES), 1).astype(F32) + 1.0
    buf, state = (buf0, buf1), (tops, sums, outs)

    dim = width // 16

    def queries(l, rows):
        rest = (mm(wqkv[l, 0:width, :], rows, NT) + twice(bcol[l, 0])).astype(BF16).astype(F32) * (dim ** -0.5 * LOG2E)
        for t in range(TERMS):
            term = rest.astype(BF16)
            rest = rest - term.astype(F32)
            for hd in range(width // dim):
                q[(TERMS * hd + t) * dim:(TERMS * hd + t + 1) * dim, :] = term[hd * dim:(hd + 1) * dim]

    def keys_values(l, i):
        cols = slice(TOK * i, TOK * (i + 1))
        rows = aall[i] if l == 0 else arecv[i]
        key = mm(wqkv[l, width:2 * width, :], rows, NT).astype(BF16)
        for hd in range(width // dim):
            for t in range(TERMS):
                kt[(TERMS * hd + t) * dim:(TERMS * hd + t + 1) * dim, cols] = key[hd * dim:(hd + 1) * dim]
        vt[:, cols] = (mm(wqkv[l, 2 * width:, :], rows, NT) + twice(bcol[l, 1])).astype(BF16)

    def rows_in(i):
        wide = dslots[i:i + GROUP].reshape(-1, CODED)
        code = wide[:, DEC:].astype(F32)
        pick = jnp.where(code == lane, 1.0, 0.0).astype(BF16)
        block = 0 if i < slots // 2 else LANES
        placed = mm(pick, z[block:block + LANES, :])
        base = jnp.where(code[:, 0:1] > 0.5, placed, token[:].astype(F32).reshape(1, -1))
        u = (base + wide[:, :DEC].astype(F32)).astype(BF16)
        if i == 0:
            h[:] = u[:TOK]
        aall[i:i + GROUP] = norm(u.astype(F32), vec[0, 0:1, :], vec[1, 0:1, :]).astype(BF16).reshape(GROUP, TOK, DEC)

    for block in blocks:
        block.wait()
    loads[0][0].wait()
    for load in loads[0][1:] + loads[1]:
        load.start()
    for i in range(0, slots, GROUP):
        rows_in(i)
    queries(0, aall[0])
    for i in range(slots):
        keys_values(0, i)
    attend(q, kt, vt, att, buf, peak, state, dim, range(slots), True, True)
    for load in loads[0][1:]:
        load.wait()
    gather = Halves(own, arecv, gsend, grecv)
    ways = (slice(0, LANES), slice(LANES, TOK))
    for n, rows in enumerate(ways):
        block_tail(h, att, a, g, vec, 0, wo, w1, w2, rows)
        own[rows, :] = norm(h[rows, :].astype(F32), vec[0, 1:2, :], vec[1, 1:2, :]).astype(BF16)
        if n == 0:
            greeted(peers)
        gather.start(n)
    arecv[0] = own[:]
    loads[1][0].wait()
    queries(1, own[:])
    keys_values(1, 0)
    for n in range(2):
        gather.own[n][2].wait_recv()
    keys_values(1, 1)
    attend(q, kt, vt, att, buf, peak, state, dim, (0, 1), True, False)
    for n in range(2):
        gather.relay(n)
        keys_values(1, 2 + 2 * n)
        gather.from_mate(n)
        keys_values(1, 3 + 2 * n)
        attend(q, kt, vt, att, buf, peak, state, dim, (2 + 2 * n, 3 + 2 * n), False, False)
    gather.relay_corner()
    keys_values(1, 6)
    gather.from_mate(2)
    keys_values(1, 7)
    attend(q, kt, vt, att, buf, peak, state, dim, (6, 7), False, True)
    for load in loads[1][1:]:
        load.wait()
    block_tail(h, att, a, g, vec, 1, wo, w1, w2, slice(0, TOK))
    norm_rows(h, y_out, fin[0:1, :], fin[1:2, :], LANES)
    gather.drain()


VM = pl.BlockSpec(memory_space=pltpu.VMEM)
HB = pl.BlockSpec(memory_space=pl.ANY)


def solution(mesh):
    def local_step(patches, enc_pos, vis_mask, dec_pos, w_embed, b_embed, enc_vec, enc_wqkv, enc_wo, enc_w1, enc_w2, enc_final, w_dec_in, mask_token, dec_vec, dec_wqkv, dec_wo, dec_w1, dec_w2, dec_final, w_out):
        layers = enc_vec.shape[0]
        evec = jnp.transpose(enc_vec, (1, 0, 2))
        dvec = jnp.transpose(dec_vec, (1, 0, 2))
        ewqkv = jnp.transpose(enc_wqkv, (0, 2, 3, 4, 1)).reshape(layers, 3, ENC, ENC)
        ewo = enc_wo.reshape(layers, ENC, ENC)
        dwqkv = jnp.transpose(dec_wqkv, (0, 2, 3, 4, 1)).reshape(layers, ALL, DEC)
        dwo = dec_wo.reshape(layers, DEC, DEC)
        dma = pltpu.SemaphoreType.DMA
        chunks = ENC // TOK
        piece = (chunks, LANES, LANES)
        dall = pl.pallas_call(
            encoder_kernel,
            out_shape=jax.ShapeDtypeStruct((LANES, TOK, CODED), BF16),
            in_specs=[VM] * 2 + [HB] * 11,
            out_specs=HB,
            scratch_shapes=[
                vm(TOK, DEC), vm(TOK, ALL), vm(TOK, ENC), vmf(12, layers, ENC), vmf(2, ENC), vm(ALL, ENC),
                vm(3 * PART, ENC), vm(ENC, ENC), vm(ENC, 2 * HID), vm(2 * HID, ENC), vm(ENC, DEC), vmf(layers + 1, 12, ENC),
                vm(chunks, 2, LANES, LANES), vm(*piece), vm(*piece), vm(*piece), vm(2, 2, *piece),
                vm(TOK, ENC), vm(TOK, ENC), vm(LANES, ENC), vm(3 * PART, TOK), vm(PART, TOK), vm(PART, LANES), vmf(LANES, ENC), vm(LANES, 2 * HID),
                vm(TOK, CODED), vmf(layers, 2, PART, LANES),
                dma((6,)), dma((chunks,)), dma((layers, 6)), dma((chunks, chunks)), dma((chunks, chunks)), dma((4,)), dma((4,)), dma((9,)), dma((9,)), dma((2,)),
            ],
            compiler_params=pltpu.CompilerParams(collective_id=0, has_side_effects=True, vmem_limit_bytes=BIG),
            name="encoder",
        )(vis_mask.reshape(1, -1), b_embed, patches, enc_pos, dec_pos, evec, enc_final, w_embed, ewqkv, ewo, enc_w1, enc_w2, w_dec_in)
        y = pl.pallas_call(
            decoder_kernel,
            out_shape=jax.ShapeDtypeStruct((TOK, DEC), BF16),
            in_specs=[VM] * 3 + [HB] * 5,
            out_specs=VM,
            scratch_shapes=[
                vm(layers, ALL, DEC), vm(layers, DEC, DEC), vm(layers, DEC, KEYS), vm(layers, KEYS, DEC),
                vm(TOK, DEC), vm(8, TOK, CODED), vm(TOK, DEC), vm(TOK, DEC), vm(TOK, DEC), vm(8, TOK, DEC), vm(8, TOK, DEC),
                vm(TERMS * DEC, KEYS), vm(DEC, KEYS), vm(TERMS * DEC, TOK), vm(DEC, TOK), vm(TOK, KEYS),
                vmf(WIDE * TOK, TOK), vmf(WIDE * TOK, TOK), vmf(WIDE, 8, TOK), vmf(16, 8, TOK), vmf(16, 8, TOK), vmf(DEC, TOK), vmf(layers, 2, DEC, LANES),
                dma((layers, 4)), dma((9,)), dma((14,)), dma((14,)),
            ],
            compiler_params=pltpu.CompilerParams(collective_id=1, has_side_effects=True, vmem_limit_bytes=MID),
            name="decoder",
        )(mask_token, dvec, dec_final, dall, dwqkv, dwo, dec_w1, dec_w2)
        return jnp.dot(y, w_out, preferred_element_type=F32)

    token_rows = P(TOKEN_AXES, None)
    in_specs = (token_rows, token_rows, P(TOKEN_AXES), token_rows) + (P(),) * 17
    return jax.shard_map(local_step, mesh=mesh, in_specs=in_specs, out_specs=token_rows, check_vma=False)
```
